512 devices in a mesh: zero: 64 (over z_hi, y, core), width: 8 (over z_lo, x).
Axes of the slice: x: 4, y: 8, z: 8 (z_hi: 4, z_lo: 2; z = z_hi * 2 + z_lo), core: 2. Of those that a mesh axis runs over, the one named last changes fastest.
Arguments:
- slopes_in: float32 [512, 128, 4096], P(None, 'zero', 'width'), may hold values from -6 to 6
- moments_in: float32 [512, 128, 4096], P(None, 'zero', 'width'), may hold values from -6 to 6
- weights_in: float32 [512, 128, 4096], P(None, 'zero', 'width'), may hold values from -0.1875 to 0.1875
Outputs:
- new_weights: float32 [512, 128, 4096], P(None, 'zero', 'width')
- new_momentum: float32 [512, 128, 4096], P(None, 'zero', 'width')
The draws below stay inside these ranges and needn't reach their ends.
All inputs are finite; a program needn't handle non-finite values.
Results may differ from the reference program's by a relative error of at most 0.0001.
Values sent between devices are 32-bit elements; how exact they have to be, the bound alone decides.
A program may use at most 64 MiB of HBM per device.

```python
import jax
import jax.numpy as jnp
from jax import lax

SIDE = 128
WIDE = 4096
MATS = 512
ITERS = 3


def level_of(stream_key, shape, pieces, smallest, high):
    def one(dim, parts):
        draws = jax.random.uniform(jax.random.fold_in(jax.random.fold_in(stream_key, 6), dim), (parts,), jnp.float32, smallest / len(pieces), high / len(pieces))
        return jnp.repeat(jnp.exp(draws), shape[dim] // parts).reshape((-1,) + (1,) * (len(shape) - dim - 1))

    factor_of = one(*pieces[0])
    for cut in pieces[1:]:
        factor_of = factor_of * one(*cut)
    return factor_of


def normal_values(rng, extent, spread, limit, cuts=(), held_as=jnp.bfloat16):
    values = jax.random.normal(rng, extent, jnp.float32) * spread
    if len(cuts) > 0:
        values = level_of(rng, extent, cuts, -0.22, 0.18) * values
    return jnp.clip(values, min=-limit, max=limit).astype(held_as)


def setup_inputs(seed: int = 0) -> dict:
    keys = jax.random.split(jax.random.key(seed), 4)
    slopes_in = normal_values(keys[0], (MATS, SIDE, WIDE), 1.0, 6.0, ((1, 64), (2, 8)), jnp.float32)
    moments_in = normal_values(keys[1], (MATS, SIDE, WIDE), 1.0, 6.0, ((1, 64), (2, 8)), jnp.float32)
    weights_in = normal_values(keys[2], (MATS, SIDE, WIDE), 0.03, 0.1875, ((1, 64), (2, 8)), jnp.float32)
    return dict(slopes_in=slopes_in, moments_in=moments_in, weights_in=weights_in)


hold_rate = 0.8
learn_rate = 0.8
decay_rate = 0.1

def reference(slopes_in, moments_in, weights_in):
    new_momentum = hold_rate * moments_in + slopes_in
    direction = hold_rate * new_momentum + slopes_in

    def orthogonal_one(stack):
        iterate = stack[None]
        iterate = iterate * lax.rsqrt(lax.optimization_barrier(jnp.sum(iterate * iterate, axis=(1, 2), keepdims=True)) + 1e-06)
        for step in range(ITERS):
            gram = jnp.einsum('mik,mjk->mij', iterate, iterate, precision=lax.Precision.HIGHEST)
            mixed = -4.775 * gram + 2.0315 * jnp.einsum('mij,mjk->mik', gram, gram, precision=lax.Precision.HIGHEST)
            iterate = 3.4445 * iterate + jnp.einsum('mij,mjk->mik', mixed, iterate, precision=lax.Precision.HIGHEST)
        return iterate[0]
    iterate = lax.map(orthogonal_one, direction)
    new_weights = (1.0 - learn_rate * decay_rate) * weights_in - learn_rate * iterate
    return (new_weights, new_momentum)
```

```python
import functools

import jax
import jax.numpy as jnp
from jax import lax
from jax.experimental import pallas as pl
from jax.experimental.pallas import tpu as pltpu
from jax.sharding import PartitionSpec as P

MESH = pl.DeviceIdType.MESH

hold_rate = 0.8
learn_rate = 0.8
decay_rate = 0.1

NX, NY, NZ, NC = 4, 8, 8, 2
NZC = NZ * NC
HALVES = 2
ROWS = 1024


def dot(a, b, contract):
    return lax.dot_general(
        a, b, (contract, ((), ())), precision=lax.Precision.HIGHEST, preferred_element_type=jnp.float32
    )


def place():
    zero = lax.axis_index("zero")
    width = lax.axis_index("width")
    core = lax.rem(zero, NC)
    y = lax.rem(zero // NC, NY)
    z = (zero // (NC * NY)) * 2 + width // NX
    x = lax.rem(width, NX)
    return x, y, z, core


def device(x, y, z, core):
    return (((z // 2) * NY + y) * NC + core, lax.rem(z, 2) * NX + x)


def ring_step(k, n):
    d = k // 2 + 1
    return d + lax.rem(k, 2) * (n - 2 * d)


def kernel(
    slopes, moments, weights, out, momentum,
    sl, mo, we, direct, t1, t2, r1, r2, xs, gs, gr, v1, v2, w1, w2, final,
    in_sem, y_send, y_recv, z_send, z_recv, x_send, x_recv,
):
    x, y, z, core = place()
    zc = z * NC + core

    def y_partner(k):
        return lax.rem(y + ring_step(k, NY), NY)

    def z_partner(k):
        pair = k // 2
        far = lax.rem(z + ring_step(pair, NZ), NZ)
        last = k // 14
        pz = far + last * (z - far)
        pc = lax.rem(core + lax.rem(k, 2) + last, NC)
        return pz, pc

    loads = []
    for u in range(2 * HALVES):
        rows = pl.ds(u * ROWS, ROWS)
        loads.append((
            pltpu.make_async_copy(slopes.at[rows], sl.at[rows], in_sem.at[u, 0]),
            pltpu.make_async_copy(moments.at[rows], mo.at[rows], in_sem.at[u, 1]),
        ))
    for a, b in loads:
        a.start()
        b.start()
    load_weights = pltpu.make_async_copy(weights, we, in_sem.at[2 * HALVES, 0])
    load_weights.start()

    barrier = pltpu.get_barrier_semaphore()

    def greet_y(k, carry):
        pl.semaphore_signal(barrier, inc=1, device_id=device(x, y_partner(k), z, core), device_id_type=MESH)
        return carry

    def greet_z(k, carry):
        pz, pc = z_partner(k)
        pl.semaphore_signal(barrier, inc=1, device_id=device(x, y, pz, pc), device_id_type=MESH)
        return carry

    def greet_x(k, carry):
        px = lax.rem(x + 1 + k, NX)
        pl.semaphore_signal(barrier, inc=1, device_id=device(px, y, z, core), device_id_type=MESH)
        return carry

    lax.fori_loop(0, NY - 1, greet_y, 0)
    lax.fori_loop(0, NZC - 1, greet_z, 0)
    lax.fori_loop(0, NX - 1, greet_x, 0)
    pl.semaphore_wait(barrier, (NY - 1) + (NZC - 1) + (NX - 1))

    def y_copy(s, k, src, dst):
        p = y_partner(k)
        return pltpu.make_async_remote_copy(
            src_ref=src(p), dst_ref=dst(y), send_sem=y_send.at[s, k], recv_sem=y_recv.at[s, k],
            device_id=device(x, p, z, core), device_id_type=MESH)

    def z_copy(s, k, src, dst):
        pz, pc = z_partner(k)
        return pltpu.make_async_remote_copy(
            src_ref=src(pz * NC + pc), dst_ref=dst(zc), send_sem=z_send.at[s, k], recv_sem=z_recv.at[s, k],
            device_id=device(x, y, pz, pc), device_id_type=MESH)

    def x_copy(h, k):
        px = lax.rem(x + 1 + k, NX)
        return pltpu.make_async_remote_copy(
            src_ref=gs.at[h], dst_ref=gr.at[h, x], send_sem=x_send.at[h, k], recv_sem=x_recv.at[h, k],
            device_id=device(px, y, z, core), device_id_type=MESH)

    def start(copy, steps, *args):
        def body(k, carry):
            copy(args[0], k, *args[1:]).start()
            return carry
        lax.fori_loop(0, steps, body, 0)

    def wait_recv(copy, steps, *args):
        def body(k, carry):
            copy(args[0], k, *args[1:]).wait_recv()
            return carry
        lax.fori_loop(0, steps, body, 0)

    def wait_send(copy, steps, *args):
        def body(k, carry):
            copy(args[0], k, *args[1:]).wait_send()
            return carry
        lax.fori_loop(0, steps, body, 0)

    def out1_a(h):
        return y_copy, NY - 1, 4 * h + 0, lambda p: direct.at[2 * h, pl.ds(p * 128, 128)], lambda p: t1.at[h, p]

    def out1_b(h):
        return z_copy, NZC - 1, 4 * h + 0, lambda p: direct.at[2 * h + 1, pl.ds(p * 64, 64)], lambda p: t2.at[h, p]

    def out2_a(h):
        return (z_copy, NZC - 1, 4 * h + 1, lambda p: t1.at[h, :, pl.ds(p * 8, 8)],
                lambda p: r1.at[h, p])

    def out2_b(h):
        return (y_copy, NY - 1, 4 * h + 1, lambda p: t2.at[h, :, pl.ds(p * 8, 8)],
                lambda p: r2.at[h, p])

    def back1_a(h):
        return z_copy, NZC - 1, 4 * h + 2, lambda p: v1.at[h, p], lambda p: w1.at[h, p]

    def back1_b(h):
        return y_copy, NY - 1, 4 * h + 2, lambda p: v2.at[h, p], lambda p: w2.at[h, p]

    def back2_a(h):
        return (y_copy, NY - 1, 4 * h + 3, lambda p: w1.at[h, :, p],
                lambda p: final.at[2 * h, pl.ds(p * 16, 16)])

    def back2_b(h):
        return (z_copy, NZC - 1, 4 * h + 3, lambda p: w2.at[h, :, p],
                lambda p: final.at[2 * h + 1, pl.ds(p * 8, 8)])

    for h in range(HALVES):
        for colour in range(2):
            u = 2 * h + colour
            loads[u][0].wait()
            loads[u][1].wait()
            rows = pl.ds(u * ROWS, ROWS)
            slope = sl[rows, :]
            fresh = hold_rate * mo[rows, :] + slope
            momentum[rows, :] = fresh
            direct[u] = hold_rate * fresh + slope
        start(*out1_a(h))
        start(*out1_b(h))
        t1[h, y] = direct[2 * h, pl.ds(pl.multiple_of(y * 128, 128), 128)]
        t2[h, zc] = direct[2 * h + 1, pl.ds(pl.multiple_of(zc * 64, 64), 64)]

    for h in range(HALVES):
        wait_recv(*out1_a(h))
        start(*out2_a(h))
        r1[h, zc] = t1[h, :, pl.ds(pl.multiple_of(zc * 8, 8), 8)]
        wait_recv(*out1_b(h))
        start(*out2_b(h))
        r2[h, y] = t2[h, :, pl.ds(pl.multiple_of(y * 8, 8), 8)]

    row_id = lax.broadcasted_iota(jnp.int32, (128, 128), 0)
    col_id = lax.broadcasted_iota(jnp.int32, (128, 128), 1)
    eye = (row_id == col_id).astype(jnp.float32)

    for h in range(HALVES):
        wait_recv(*out2_a(h))
        flat = r1.at[h].reshape(ROWS, 128)
        for zl in range(2):
            for ct in range(4):
                for row in range(2):
                    for zh in range(4):
                        xs[2 * h, pl.ds(row * 64 + zh * 16, 16), pl.ds((zl * 4 + ct) * 128, 128)] = flat[
                            pl.ds(zh * 256 + zl * 128 + ct * 2 + row, 16, stride=8), :]
        a = xs[2 * h]
        gs[h, 0] = dot(a, a, ((1,), (1,)))
        wait_recv(*out2_b(h))
        flat = r2.at[h].reshape(ROWS, 128)
        for zl in range(2):
            for ct in range(4):
                for row in range(2):
                    for zh in range(4):
                        for c in range(2):
                            xs[2 * h + 1, pl.ds(row * 64 + zh * 16 + c * 8, 8), pl.ds((zl * 4 + ct) * 128, 128)] = flat[
                                pl.ds(zh * 32 + zl * 16 + c * 8 + ct * 2 + row, 8, stride=128), :]
        a = xs[2 * h + 1]
        gs[h, 1] = dot(a, a, ((1,), (1,)))
        for k in range(NX - 1):
            x_copy(h, k).start()
        gr[h, x] = gs[h]
        for k in range(NX - 1):
            x_copy(h, k).wait_recv()
        for i in range(2):
            gram = (gr[h, 0, i] + gr[h, 1, i]) + (gr[h, 2, i] + gr[h, 3, i])
            scale = lax.rsqrt(jnp.sum(jnp.sum(gram * eye, axis=1, keepdims=True), axis=0, keepdims=True) + 1e-06)
            gram = gram * (scale * scale)
            total = scale * eye
            for step in range(3):
                mixed = 3.4445 * eye - 4.775 * gram + 2.0315 * dot(gram, gram, ((1,), (0,)))
                total = scale * mixed if step == 0 else dot(mixed, total, ((1,), (0,)))
                if step < 2:
                    gram = dot(dot(mixed, gram, ((1,), (0,))), mixed, ((1,), (0,)))
            new = dot(total, xs[2 * h + i], ((1,), (0,)))
            if i == 0:
                flat = v1.at[h].reshape(ROWS, 128)
                for zl in range(2):
                    for ct in range(4):
                        for row in range(2):
                            for zh in range(4):
                                flat[pl.ds(zh * 256 + zl * 128 + ct * 2 + row, 16, stride=8), :] = new[
                                    row * 64 + zh * 16:row * 64 + zh * 16 + 16, (zl * 4 + ct) * 128:(zl * 4 + ct + 1) * 128]
                start(*back1_a(h))
                w1[h, zc] = v1[h, zc]
            else:
                flat = v2.at[h].reshape(ROWS, 128)
                for zl in range(2):
                    for ct in range(4):
                        for row in range(2):
                            for zh in range(4):
                                for c in range(2):
                                    first = row * 64 + zh * 16 + c * 8
                                    flat[pl.ds(zh * 32 + zl * 16 + c * 8 + ct * 2 + row, 8, stride=128), :] = new[
                                        first:first + 8, (zl * 4 + ct) * 128:(zl * 4 + ct + 1) * 128]
                start(*back1_b(h))
                w2[h, y] = v2[h, y]

    for h in range(HALVES):
        wait_recv(*back1_b(h))
        start(*back2_b(h))
        final[2 * h + 1, pl.ds(zc * 8, 8)] = w2[h, :, zc]
        wait_recv(*back1_a(h))
        start(*back2_a(h))
        final[2 * h, pl.ds(y * 16, 16)] = w1[h, :, y]

    load_weights.wait()
    for h in range(HALVES):
        for colour, plan in ((0, back2_a), (1, back2_b)):
            wait_recv(*plan(h))
            u = 2 * h + colour
            rows = pl.ds(u * ROWS, ROWS)
            out[rows, :] = (1.0 - learn_rate * decay_rate) * we[rows, :] - learn_rate * final[u].reshape(ROWS, 128)

    for h in range(HALVES):
        for plan in (out1_a, out1_b, out2_a, out2_b, back1_a, back1_b, back2_a, back2_b):
            wait_send(*plan(h))
        for k in range(NX - 1):
            x_copy(h, k).wait_send()


def body(slopes_in, moments_in, weights_in):
    mats, side, wide = slopes_in.shape

    def flat(a):
        return a.reshape(mats, side, wide // 128, 128).transpose(0, 2, 1, 3).reshape(mats * side * wide // 128, 128)

    def whole(a):
        return a.reshape(mats, wide // 128, side, 128).transpose(0, 2, 1, 3).reshape(mats, side, wide)

    f32 = jnp.float32
    shape = (mats * side * wide // 128, 128)
    vmem = pltpu.VMEM
    dma = pltpu.SemaphoreType.DMA
    out, momentum = pl.pallas_call(
        kernel,
        out_shape=(jax.ShapeDtypeStruct(shape, f32),) * 2,
        in_specs=[pl.BlockSpec(memory_space=pltpu.HBM)] * 3,
        out_specs=[pl.BlockSpec(memory_space=pltpu.VMEM)] * 2,
        scratch_shapes=[
            vmem(shape, f32), vmem(shape, f32), vmem(shape, f32),
            vmem((4, ROWS, 128), f32),
            vmem((HALVES, NY, 128, 128), f32), vmem((HALVES, NZC, 64, 128), f32),
            vmem((HALVES, NZC, NY, 8, 128), f32), vmem((HALVES, NY, NZC, 8, 128), f32),
            vmem((2 * HALVES, 128, 1024), f32),
            vmem((HALVES, 2, 128, 128), f32), vmem((HALVES, NX, 2, 128, 128), f32),
            vmem((HALVES, NZC, NY, 8, 128), f32), vmem((HALVES, NY, NZC, 8, 128), f32),
            vmem((HALVES, NZC, NY, 8, 128), f32), vmem((HALVES, NY, NZC, 8, 128), f32),
            vmem((4, 128, 8, 128), f32),
            dma((2 * HALVES + 1, 2)),
            dma((4 * HALVES, NY - 1)), dma((4 * HALVES, NY - 1)),
            dma((4 * HALVES, NZC - 1)), dma((4 * HALVES, NZC - 1)),
            dma((HALVES, NX - 1)), dma((HALVES, NX - 1)),
        ],
        compiler_params=pltpu.CompilerParams(
            collective_id=0, has_side_effects=True, vmem_limit_bytes=48 * 1024 * 1024),
        name="exchange",
    )(flat(slopes_in), flat(moments_in), flat(weights_in))
    return whole(out), whole(momentum)


def solution(mesh):
    spec = P(None, "zero", "width")
    return jax.shard_map(body, mesh=mesh, in_specs=(spec,) * 3, out_specs=(spec,) * 2, check_vma=False)
```

```python
import functools

import jax
import jax.numpy as jnp
from jax import lax
from jax.experimental import pallas as pl
from jax.experimental.pallas import tpu as pltpu
from jax.sharding import PartitionSpec as P

MESH = pl.DeviceIdType.MESH

hold_rate = 0.8
learn_rate = 0.8
decay_rate = 0.1

NX, NY, NZ, NC = 4, 8, 8, 2
NZC = NZ * NC
HALVES = 2
ROWS = 1024


def dot(a, b, contract):
    return lax.dot_general(
        a, b, (contract, ((), ())), precision=lax.Precision.HIGHEST, preferred_element_type=jnp.float32
    )


def place():
    zero = lax.axis_index("zero")
    width = lax.axis_index("width")
    core = lax.rem(zero, NC)
    y = lax.rem(zero // NC, NY)
    z = (zero // (NC * NY)) * 2 + width // NX
    x = lax.rem(width, NX)
    return x, y, z, core


def device(x, y, z, core):
    return (((z // 2) * NY + y) * NC + core, lax.rem(z, 2) * NX + x)


def ring_step(k, n):
    d = (n - k) // 2
    return d + lax.rem(k, 2) * (n - 2 * d)


def kernel(
    slopes, moments, weights, out, momentum,
    sl, mo, we, direct, t1, t2, r1, r2, xs, gs, gr, v1, v2, w1, w2, final,
    in_sem, y_send, y_recv, z_send, z_recv, x_send, x_recv,
):
    x, y, z, core = place()
    zc = z * NC + core

    def y_partner(k):
        return lax.rem(y + ring_step(k, NY), NY)

    def z_partner(k):
        pair = k // 2
        far = lax.rem(z + ring_step(pair, NZ), NZ)
        last = k // 14
        pz = far + last * (z - far)
        pc = lax.rem(core + lax.rem(k, 2) + last, NC)
        return pz, pc

    barrier = pltpu.get_barrier_semaphore()

    def greet_y(k, carry):
        pl.semaphore_signal(barrier, inc=1, device_id=device(x, y_partner(k), z, core), device_id_type=MESH)
        return carry

    def greet_z(k, carry):
        pz, pc = z_partner(k)
        pl.semaphore_signal(barrier, inc=1, device_id=device(x, y, pz, pc), device_id_type=MESH)
        return carry

    def greet_x(k, carry):
        px = lax.rem(x + 1 + k, NX)
        pl.semaphore_signal(barrier, inc=1, device_id=device(px, y, z, core), device_id_type=MESH)
        return carry

    lax.fori_loop(0, NZC - 1, greet_z, 0)
    lax.fori_loop(0, NY - 1, greet_y, 0)
    lax.fori_loop(0, NX - 1, greet_x, 0)
    loads = []
    for u in range(2 * HALVES):
        rows = pl.ds(u * ROWS, ROWS)
        loads.append((
            pltpu.make_async_copy(slopes.at[rows], sl.at[rows], in_sem.at[u, 0]),
            pltpu.make_async_copy(moments.at[rows], mo.at[rows], in_sem.at[u, 1]),
        ))
    for a, b in loads:
        a.start()
        b.start()
    load_weights = pltpu.make_async_copy(weights, we, in_sem.at[2 * HALVES, 0])
    load_weights.start()


    def y_copy(s, k, src, dst):
        p = y_partner(k)
        return pltpu.make_async_remote_copy(
            src_ref=src(p), dst_ref=dst(y), send_sem=y_send.at[s], recv_sem=y_recv.at[s],
            device_id=device(x, p, z, core), device_id_type=MESH)

    def z_copy(s, k, src, dst):
        pz, pc = z_partner(k)
        return pltpu.make_async_remote_copy(
            src_ref=src(pz * NC + pc), dst_ref=dst(zc), send_sem=z_send.at[s], recv_sem=z_recv.at[s],
            device_id=device(x, y, pz, pc), device_id_type=MESH)

    def x_copy(s, px):
        return pltpu.make_async_remote_copy(
            src_ref=gs.at[s], dst_ref=gr.at[s, x], send_sem=x_send.at[s], recv_sem=x_recv.at[s],
            device_id=device(px, y, z, core), device_id_type=MESH)

    def x_all(s):
        whole = gr.at[s, pl.ds(0, NX - 1)]
        return pltpu.make_async_remote_copy(
            src_ref=whole, dst_ref=whole, send_sem=x_send.at[s], recv_sem=x_recv.at[s],
            device_id=device(lax.rem(x + 1, NX), y, z, core), device_id_type=MESH)

    def start(copy, steps, slot, src, dst, whole):
        def body(k, carry):
            copy(slot, k, src, dst).start()
            return carry
        lax.fori_loop(0, steps, body, 0)

    def wait_recv(copy, steps, slot, src, dst, whole):
        copy(slot, 0, lambda p: whole, lambda p: whole).wait_recv()

    def wait_send(copy, steps, slot, src, dst, whole):
        copy(slot, 0, lambda p: whole, lambda p: whole).wait_send()

    def out1_a(h):
        return (y_copy, NY - 1, 4 * h, lambda p: direct.at[2 * h, pl.ds(p * 128, 128)], lambda p: t1.at[h, p],
                t1.at[h, pl.ds(0, NY - 1)])

    def out1_b(h):
        return (z_copy, NZC - 1, 4 * h, lambda p: direct.at[2 * h + 1, pl.ds(p * 64, 64)], lambda p: t2.at[h, p],
                t2.at[h, pl.ds(0, NZC - 1)])

    def out2_a(h):
        return (z_copy, NZC - 1, 4 * h + 1, lambda p: t1.at[h, :, pl.ds(p * 8, 8)], lambda p: r1.at[h, p],
                r1.at[h, pl.ds(0, NZC - 1)])

    def out2_b(h):
        return (y_copy, NY - 1, 4 * h + 1, lambda p: t2.at[h, :, pl.ds(p * 8, 8)], lambda p: r2.at[h, p],
                r2.at[h, pl.ds(0, NY - 1)])

    def back1_a(h):
        return (z_copy, NZC - 1, 4 * h + 2, lambda p: v1.at[h, p], lambda p: w1.at[h, p],
                w1.at[h, pl.ds(0, NZC - 1)])

    def back1_b(h):
        return (y_copy, NY - 1, 4 * h + 2, lambda p: v2.at[h, p], lambda p: w2.at[h, p],
                w2.at[h, pl.ds(0, NY - 1)])

    def back2_a(h):
        return (y_copy, NY - 1, 4 * h + 3, lambda p: w1.at[h, :, p], lambda p: final.at[2 * h, pl.ds(p * 16, 16)],
                final.at[2 * h, pl.ds(0, 16 * (NY - 1))])

    def back2_b(h):
        return (z_copy, NZC - 1, 4 * h + 3, lambda p: w2.at[h, :, p], lambda p: final.at[2 * h + 1, pl.ds(p * 8, 8)],
                final.at[2 * h + 1, pl.ds(0, 8 * (NZC - 1))])

    def take(h, i):
        flat = (r1, r2)[i].at[h].reshape(ROWS, 128)
        for zl in range(2):
            for ct in range(4):
                columns = pl.ds((zl * 4 + ct) * 128, 128)
                for row in range(2):
                    for zh in range(4):
                        if i == 0:
                            xs[2 * h, pl.ds(row * 64 + zh * 16, 16), columns] = flat[
                                pl.ds(zh * 256 + zl * 128 + ct * 2 + row, 16, stride=8), :]
                        else:
                            for c in range(2):
                                xs[2 * h + 1, pl.ds(row * 64 + zh * 16 + c * 8, 8), columns] = flat[
                                    pl.ds(zh * 32 + zl * 16 + c * 8 + ct * 2 + row, 8, stride=128), :]

    def give(h, i, new):
        flat = (v1, v2)[i].at[h].reshape(ROWS, 128)
        for zl in range(2):
            for ct in range(4):
                tile = new[:, (zl * 4 + ct) * 128:(zl * 4 + ct + 1) * 128]
                for row in range(2):
                    for zh in range(4):
                        first = row * 64 + zh * 16
                        if i == 0:
                            flat[pl.ds(zh * 256 + zl * 128 + ct * 2 + row, 16, stride=8), :] = tile[first:first + 16]
                        else:
                            for c in range(2):
                                flat[pl.ds(zh * 32 + zl * 16 + c * 8 + ct * 2 + row, 8, stride=128), :] = tile[
                                    first + c * 8:first + c * 8 + 8]

    def renew(u, first, rows):
        at = pl.ds(pl.multiple_of(u * ROWS + first, 8), rows)
        fresh = final[u, pl.ds(first // 8, rows // 8)].reshape(rows, 128)
        out[at, :] = (1.0 - learn_rate * decay_rate) * we[at, :] - learn_rate * fresh

    for u in range(2 * HALVES):
        loads[u][0].wait()
        loads[u][1].wait()
        rows = pl.ds(u * ROWS, ROWS)
        slope = sl[rows, :]
        fresh = hold_rate * mo[rows, :] + slope
        momentum[rows, :] = fresh
        direct[u] = hold_rate * fresh + slope
    pl.semaphore_wait(barrier, (NY - 1) + (NZC - 1) + (NX - 1))
    for h in range(HALVES):
        start(*out1_a(h))
        start(*out1_b(h))
    for h in range(HALVES):
        t1[h, y] = direct[2 * h, pl.ds(pl.multiple_of(y * 128, 128), 128)]
        t2[h, zc] = direct[2 * h + 1, pl.ds(pl.multiple_of(zc * 64, 64), 64)]

    for h in range(HALVES):
        wait_recv(*out1_a(h))
        start(*out2_a(h))
        wait_recv(*out1_b(h))
        start(*out2_b(h))
        r1[h, zc] = t1[h, :, pl.ds(pl.multiple_of(zc * 8, 8), 8)]
        r2[h, y] = t2[h, :, pl.ds(pl.multiple_of(y * 8, 8), 8)]

    row_id = lax.broadcasted_iota(jnp.int32, (128, 128), 0)
    col_id = lax.broadcasted_iota(jnp.int32, (128, 128), 1)
    eye = (row_id == col_id).astype(jnp.float32)
    inner = ((1,), (0,))

    for h in range(HALVES):
        for i, plan in enumerate((out2_a, out2_b)):
            wait_recv(*plan(h))
            take(h, i)
            a = xs[2 * h + i]
            gs[2 * h + i] = dot(a, a, ((1,), (1,)))
            for k in (2, 1, 3):
                x_copy(2 * h + i, lax.rem(x + k, NX)).start()
            gr[2 * h + i, x] = gs[2 * h + i]
        if h > 0:
            wait_recv(*back1_a(h - 1))
            start(*back2_a(h - 1))
            wait_recv(*back1_b(h - 1))
            start(*back2_b(h - 1))
        grams, scales, totals = [], [], []
        for i in range(2):
            at = 2 * h + i
            x_all(at).wait_recv()
            gram = (gr[at, 0] + gr[at, 1]) + (gr[at, 2] + gr[at, 3])
            scale = lax.rsqrt(jnp.sum(jnp.sum(gram * eye, axis=1, keepdims=True), axis=0, keepdims=True) + 1e-06)
            scales.append(scale)
            grams.append(gram * (scale * scale))
        for step in range(3):
            mixes = [3.4445 * eye - 4.775 * g + 2.0315 * dot(g, g, inner) for g in grams]
            if step == 0:
                totals = [s * m for s, m in zip(scales, mixes)]
            if step < 2:
                halves = [dot(m, g, inner) for m, g in zip(mixes, grams)]
                grams = [dot(a, m, inner) for a, m in zip(halves, mixes)]
            if step > 0:
                totals = [dot(m, t, inner) for m, t in zip(mixes, totals)]
        for i, plan in enumerate((back1_a, back1_b)):
            give(h, i, dot(totals[i], xs[2 * h + i], inner))
            start(*plan(h))
            if i == 0:
                w1[h, zc] = v1[h, zc]
            else:
                w2[h, y] = v2[h, y]

    h = HALVES - 1
    for plan in (back1_a, back1_b):
        wait_recv(*plan(h))
        start(*((back2_a, back2_b)[plan is back1_b](h)))
    load_weights.wait()
    for g in range(HALVES):
        final[2 * g, pl.ds(y * 16, 16)] = w1[g, :, y]
        final[2 * g + 1, pl.ds(zc * 8, 8)] = w2[g, :, zc]
        renew(2 * g, y * 128, 128)
        renew(2 * g + 1, zc * 64, 64)
    for g in range(HALVES):
        for plan in (out1_a, out1_b, out2_a, out2_b):
            wait_send(*plan(g))
        for i in range(2):
            x_all(2 * g + i).wait_send()

    for g in range(HALVES):
        for plan in (back1_a, back1_b):
            wait_send(*plan(g))
    for g in range(HALVES):
        wait_recv(*back2_a(g))

        def from_y(k, carry):
            renew(2 * g, lax.rem(y + 1 + k, NY) * 128, 128)
            return carry

        lax.fori_loop(0, NY - 1, from_y, 0)
        wait_recv(*back2_b(g))

        def from_z(k, carry):
            renew(2 * g + 1, lax.rem(zc + 1 + k, NZC) * 64, 64)
            return carry

        lax.fori_loop(0, NZC - 1, from_z, 0)
    for g in range(HALVES):
        for plan in (back2_a, back2_b):
            wait_send(*plan(g))


def body(slopes_in, moments_in, weights_in):
    mats, side, wide = slopes_in.shape

    def flat(a):
        return a.reshape(mats, side, wide // 128, 128).transpose(0, 2, 1, 3).reshape(mats * side * wide // 128, 128)

    def whole(a):
        return a.reshape(mats, wide // 128, side, 128).transpose(0, 2, 1, 3).reshape(mats, side, wide)

    f32 = jnp.float32
    shape = (mats * side * wide // 128, 128)
    vmem = pltpu.VMEM
    dma = pltpu.SemaphoreType.DMA
    out, momentum = pl.pallas_call(
        kernel,
        out_shape=(jax.ShapeDtypeStruct(shape, f32),) * 2,
        in_specs=[pl.BlockSpec(memory_space=pltpu.HBM)] * 3,
        out_specs=[pl.BlockSpec(memory_space=pltpu.VMEM)] * 2,
        scratch_shapes=[
            vmem(shape, f32), vmem(shape, f32), vmem(shape, f32),
            vmem((4, ROWS, 128), f32),
            vmem((HALVES, NY, 128, 128), f32), vmem((HALVES, NZC, 64, 128), f32),
            vmem((HALVES, NZC, NY, 8, 128), f32), vmem((HALVES, NY, NZC, 8, 128), f32),
            vmem((2 * HALVES, 128, 1024), f32),
            vmem((2 * HALVES, 128, 128), f32), vmem((2 * HALVES, NX, 128, 128), f32),
            vmem((HALVES, NZC, NY, 8, 128), f32), vmem((HALVES, NY, NZC, 8, 128), f32),
            vmem((HALVES, NZC, NY, 8, 128), f32), vmem((HALVES, NY, NZC, 8, 128), f32),
            vmem((4, 128, 8, 128), f32),
            dma((2 * HALVES + 1, 2)),
            dma((4 * HALVES,)), dma((4 * HALVES,)), dma((4 * HALVES,)), dma((4 * HALVES,)),
            dma((2 * HALVES,)), dma((2 * HALVES,)),
        ],
        compiler_params=pltpu.CompilerParams(
            collective_id=0, has_side_effects=True, vmem_limit_bytes=48 * 1024 * 1024),
        name="exchange",
    )(flat(slopes_in), flat(moments_in), flat(weights_in))
    return whole(out), whole(momentum)


def solution(mesh):
    spec = P(None, "zero", "width")
    return jax.shard_map(body, mesh=mesh, in_specs=(spec,) * 3, out_specs=(spec,) * 2, check_vma=False)
```

```python
import jax
import jax.numpy as jnp
from jax import lax
from jax.experimental import pallas as pl
from jax.experimental.pallas import tpu as pltpu
from jax.sharding import PartitionSpec as P

MESH = pl.DeviceIdType.MESH

hold_rate = 0.8
learn_rate = 0.8
decay_rate = 0.1

NX, NY, NZ, NC = 4, 8, 8, 2
NZC = NZ * NC
HALVES = 2
ROWS = 1024


def dot(a, b, contract):
    return lax.dot_general(
        a, b, (contract, ((), ())), precision=lax.Precision.HIGHEST, preferred_element_type=jnp.float32
    )


def ring_step(k, n):
    d = (n - k) // 2
    return d + lax.rem(k, 2) * (n - 2 * d)


def kernel(
    slopes, moments, weights, out, momentum,
    sl, mo, we, direct, t1, t2, r1, r2, xs, gs, gr, v1, v2, w1, w2, final,
    in_sem, send_sem, recv_sem, x_send, x_recv,
):
    zero = lax.axis_index("zero")
    width = lax.axis_index("width")
    core = lax.rem(zero, NC)
    y = lax.rem(zero // NC, NY)
    zh = zero // (NC * NY)
    x = lax.rem(width, NX)
    own = (width // NX) * NC + core
    zc = zh * 4 + own

    def device(px, py, pzh, quarter):
        return ((pzh * NY + py) * NC + lax.rem(quarter, NC), (quarter // NC) * NX + px)

    def y_partner(k, back):
        d = ring_step(k, NY)
        return lax.rem(y + NY - d, NY) if back else lax.rem(y + d, NY)

    def z_partner(g, k, back):
        if g == 0:
            idx, quarter = 0, k
        elif g == 1:
            idx, quarter = 1 + 2 * lax.rem(k, 2), k // 2
        else:
            idx, quarter = 2, lax.rem(own + 1 + k, 4)
        return idx, quarter, lax.rem(zh + (idx + 2 if back else 6 - idx), 4)

    Z_FAR, Z_NEAR = ((0, 4),), ((1, 8), (2, 3))
    Z_ALL = Z_FAR + Z_NEAR
    Y_FAR, Y_NEAR = ((0, 3),), ((3, NY - 1),)
    Y_ALL = ((0, NY - 1),)

    def loop(lo, hi, step):
        def body(k, carry):
            step(k)
            return carry
        lax.fori_loop(lo, hi, body, 0)

    loads = []
    for u in range(2 * HALVES):
        rows = pl.ds(u * ROWS, ROWS)
        loads.append((
            pltpu.make_async_copy(slopes.at[rows], sl.at[rows], in_sem.at[u, 0]),
            pltpu.make_async_copy(moments.at[rows], mo.at[rows], in_sem.at[u, 1]),
        ))
    for a, b in loads:
        a.start()
        b.start()

    barrier = pltpu.get_barrier_semaphore()

    def greet(target):
        pl.semaphore_signal(barrier, inc=1, device_id=target, device_id_type=MESH)

    for g, n in Z_ALL:
        def greet_z(k):
            _, quarter, pzh = z_partner(g, k, False)
            greet(device(x, y, pzh, quarter))
        loop(0, n, greet_z)
    loop(0, NY - 1, lambda k: greet(device(x, y_partner(k, False), zh, own)))
    loop(1, NX, lambda k: greet(device(lax.rem(x + k, NX), y, zh, own)))

    load_weights = pltpu.make_async_copy(weights, we, in_sem.at[2 * HALVES, 0])
    load_weights.start()

    def remote(s, src, dst, target):
        return pltpu.make_async_remote_copy(
            src_ref=src, dst_ref=dst, send_sem=send_sem.at[s], recv_sem=recv_sem.at[s],
            device_id=target, device_id_type=MESH)

    class Along:
        def __init__(self, axis, s, groups, back, src, dst, whole):
            self.axis, self.s, self.groups, self.back = axis, s, groups, back
            self.src, self.dst, self.whole = src, dst, whole

        def copy(self, g, k):
            if self.axis == "y":
                p = y_partner(k, self.back)
                return remote(self.s, self.src(k, p), self.dst(k), device(x, p, zh, own))
            idx, quarter, pzh = z_partner(g, k, self.back)
            return remote(self.s, self.src(idx * 4 + quarter, pzh * 4 + quarter), self.dst(idx * 4 + own),
                          device(x, y, pzh, quarter))

        def start(self):
            for g, n in self.groups:
                if self.axis == "y":
                    loop(g, n, lambda k: self.copy(0, k).start())
                else:
                    loop(0, n, lambda k: self.copy(g, k).start())

        def all(self):
            return remote(self.s, self.whole, self.whole, device(x, lax.rem(y + 1, NY), zh, own))

    def x_copy(s, px):
        return pltpu.make_async_remote_copy(
            src_ref=gs.at[s], dst_ref=gr.at[s, x], send_sem=x_send.at[s], recv_sem=x_recv.at[s],
            device_id=device(px, y, zh, own), device_id_type=MESH)

    def x_all(s):
        whole = gr.at[s, pl.ds(0, NX - 1)]
        return pltpu.make_async_remote_copy(
            src_ref=whole, dst_ref=whole, send_sem=x_send.at[s], recv_sem=x_recv.at[s],
            device_id=device(lax.rem(x + 1, NX), y, zh, own), device_id_type=MESH)

    out1, out2, back1, back2 = [], [], [], []
    for h in range(HALVES):
        a, b = 2 * h, 2 * h + 1
        out1.append((
            Along("y", 12 * h, Y_ALL, False, lambda k, p, a=a: direct.at[a, pl.ds(p * 128, 128)],
                  lambda k, h=h: t1.at[h, k], t1.at[h, pl.ds(0, NY - 1)]),
            Along("z", 12 * h + 1, Z_ALL, False, lambda k, p, b=b: direct.at[b, pl.ds(p * 64, 64)],
                  lambda k, h=h: t2.at[h, k], t2.at[h, pl.ds(0, NZC - 1)]),
        ))
        out2.append((
            Along("z", 12 * h + 2, Z_ALL, False, lambda k, p, h=h: t1.at[h, :, pl.ds(p * 8, 8)],
                  lambda k, h=h: r1.at[h, zc], r1.at[h, pl.ds(0, NZC - 1)]),
            Along("y", 12 * h + 3, Y_ALL, False, lambda k, p, h=h: t2.at[h, :, pl.ds(p * 8, 8)],
                  lambda k, h=h: r2.at[h, y], r2.at[h, pl.ds(0, NY - 1)]),
        ))
        back1.append([])
        back2.append([])
        for part in range(2):
            ya, yb = (pl.ds(0, 3), pl.ds(3, 5))[part], (pl.ds(0, 4), pl.ds(4, 12))[part]
            s = 12 * h + 4 + 4 * part
            back1[h].append((
                Along("z", s, Z_ALL, False, lambda k, p, h=h, ya=ya: v1.at[h, p, ya],
                      lambda k, h=h, ya=ya: w1.at[h, zc, ya], w1.at[h, pl.ds(0, NZC - 1), ya]),
                Along("y", s + 1, Y_ALL, False, lambda k, p, h=h, yb=yb: v2.at[h, p, yb],
                      lambda k, h=h, yb=yb: w2.at[h, y, yb], w2.at[h, pl.ds(0, NY - 1), yb]),
            ))
            back2[h].append((
                Along("y", s + 2, (Y_FAR, Y_NEAR)[part], True, lambda k, p, h=h: w1.at[h, :, k],
                      lambda k, a=a: final.at[a, pl.ds(y * 16, 16)], final.at[a, pl.ds(0, (48, 64)[part])]),
                Along("z", s + 3, (Z_FAR, Z_NEAR)[part], True, lambda k, p, h=h: w2.at[h, :, k],
                      lambda k, b=b: final.at[b, pl.ds(zc * 8, 8)], final.at[b, pl.ds(0, (32, 88)[part])]),
            ))

    def take(h, i):
        flat = (r1, r2)[i].at[h].reshape(ROWS, 128)
        for zl in range(2):
            for ct in range(4):
                columns = pl.ds((zl * 4 + ct) * 128, 128)
                for row in range(2):
                    for zh in range(4):
                        if i == 0:
                            xs[2 * h, pl.ds(row * 64 + zh * 16, 16), columns] = flat[
                                pl.ds(zh * 256 + zl * 128 + ct * 2 + row, 16, stride=8), :]
                        else:
                            for c in range(2):
                                xs[2 * h + 1, pl.ds(row * 64 + zh * 16 + c * 8, 8), columns] = flat[
                                    pl.ds(zh * 32 + zl * 16 + c * 8 + ct * 2 + row, 8, stride=128), :]

    def give(h, i, new):
        flat = (v1, v2)[i].at[h].reshape(ROWS, 128)
        for zl in range(2):
            for ct in range(4):
                tile = new[:, (zl * 4 + ct) * 128:(zl * 4 + ct + 1) * 128]
                for row in range(2):
                    for zh in range(4):
                        first = row * 64 + zh * 16
                        if i == 0:
                            flat[pl.ds(zh * 256 + zl * 128 + ct * 2 + row, 16, stride=8), :] = tile[first:first + 16]
                        else:
                            for c in range(2):
                                flat[pl.ds(zh * 32 + zl * 16 + c * 8 + ct * 2 + row, 8, stride=128), :] = tile[
                                    first + c * 8:first + c * 8 + 8]

    def renew(u, first, rows):
        at = pl.ds(pl.multiple_of(u * ROWS + first, 8), rows)
        fresh = final[u, pl.ds(first // 8, rows // 8)].reshape(rows, 128)
        out[at, :] = (1.0 - learn_rate * decay_rate) * we[at, :] - learn_rate * fresh

    for u in range(2 * HALVES):
        loads[u][0].wait()
        loads[u][1].wait()
        rows = pl.ds(u * ROWS, ROWS)
        slope = sl[rows, :]
        fresh = hold_rate * mo[rows, :] + slope
        momentum[rows, :] = fresh
        direct[u] = hold_rate * fresh + slope
        if u == 0:
            pl.semaphore_wait(barrier, (NY - 1) + (NZC - 1) + (NX - 1))
        out1[u // 2][u % 2].start()
    for h in range(HALVES):
        t1[h, NY - 1] = direct[2 * h, pl.ds(pl.multiple_of(y * 128, 128), 128)]
        t2[h, 8 + own] = direct[2 * h + 1, pl.ds(pl.multiple_of(zc * 64, 64), 64)]

    for h in range(HALVES):
        for i in range(2):
            out1[h][i].all().wait_recv()
            out2[h][i].start()
        r1[h, zc] = t1[h, :, pl.ds(pl.multiple_of(zc * 8, 8), 8)]
        r2[h, y] = t2[h, :, pl.ds(pl.multiple_of(y * 8, 8), 8)]

    row_id = lax.broadcasted_iota(jnp.int32, (128, 128), 0)
    col_id = lax.broadcasted_iota(jnp.int32, (128, 128), 1)
    eye = (row_id == col_id).astype(jnp.float32)
    inner = ((1,), (0,))

    def forward(h):
        for part in range(2):
            for i in range(2):
                back1[h][part][i].all().wait_recv()
                back2[h][part][i].start()

    for h in range(HALVES):
        for i in range(2):
            out2[h][i].all().wait_recv()
            take(h, i)
            a = xs[2 * h + i]
            gs[2 * h + i] = dot(a, a, ((1,), (1,)))
            for k in (2, 1, 3):
                x_copy(2 * h + i, lax.rem(x + k, NX)).start()
            gr[2 * h + i, x] = gs[2 * h + i]
        if h > 0:
            forward(h - 1)
        grams, scales, totals = [], [], []
        for i in range(2):
            at = 2 * h + i
            x_all(at).wait_recv()
            gram = (gr[at, 0] + gr[at, 1]) + (gr[at, 2] + gr[at, 3])
            scale = lax.rsqrt(jnp.sum(jnp.sum(gram * eye, axis=1, keepdims=True), axis=0, keepdims=True) + 1e-06)
            scales.append(scale)
            grams.append(gram * (scale * scale))
        for step in range(3):
            mixes = [3.4445 * eye - 4.775 * g + 2.0315 * dot(g, g, inner) for g in grams]
            if step == 0:
                totals = [s * m for s, m in zip(scales, mixes)]
            if step < 2:
                halves = [dot(m, g, inner) for m, g in zip(mixes, grams)]
                grams = [dot(a, m, inner) for a, m in zip(halves, mixes)]
            if step > 0:
                totals = [dot(m, t, inner) for m, t in zip(mixes, totals)]
        for i in range(2):
            give(h, i, dot(totals[i], xs[2 * h + i], inner))
            for part in range(2):
                back1[h][part][i].start()
            if i == 0:
                w1[h, zc] = v1[h, zc]
            else:
                w2[h, y] = v2[h, y]

    forward(HALVES - 1)
    load_weights.wait()
    for g in range(HALVES):
        final[2 * g, pl.ds(y * 16, 16)] = w1[g, :, NY - 1]
        final[2 * g + 1, pl.ds(zc * 8, 8)] = w2[g, :, 8 + own]
        renew(2 * g, y * 128, 128)
    for g in range(HALVES):
        for pair in (out1[g], out2[g], back1[g][0], back1[g][1]):
            for one in pair:
                one.all().wait_send()
        for i in range(2):
            x_all(2 * g + i).wait_send()
    for g in range(HALVES):
        for part in range(2):
            back2[g][part][0].all().wait_recv()
            for lo, hi in (Y_FAR, Y_NEAR)[part]:
                loop(lo, hi, lambda k: renew(2 * g, y_partner(k, False) * 128, 128))
            back2[g][part][1].all().wait_recv()
            for idx in ((0,), (1, 3, 2))[part]:
                renew(2 * g + 1, lax.rem(zh + 6 - idx, 4) * 256, 256)
    for g in range(HALVES):
        for pair in back2[g]:
            for one in pair:
                one.all().wait_send()


PIECES = 4


def land(out, momentum, out_hbm, momentum_hbm, sem):
    copies = []
    for i in range(PIECES):
        rows = pl.ds(i * (out.shape[0] // PIECES), out.shape[0] // PIECES)
        copies.append(pltpu.make_async_copy(out.at[rows], out_hbm.at[rows], sem.at[0, i]))
        copies.append(pltpu.make_async_copy(momentum.at[rows], momentum_hbm.at[rows], sem.at[1, i]))
    for copy in copies:
        copy.start()
    for copy in copies:
        copy.wait()


def body(slopes_in, moments_in, weights_in):
    mats, side, wide = slopes_in.shape

    def flat(a):
        return a.reshape(mats, side, wide // 128, 128).transpose(0, 2, 1, 3).reshape(mats * side * wide // 128, 128)

    def whole(a):
        return a.reshape(mats, wide // 128, side, 128).transpose(0, 2, 1, 3).reshape(mats, side, wide)

    f32 = jnp.float32
    shape = (mats * side * wide // 128, 128)
    vmem = pltpu.VMEM
    dma = pltpu.SemaphoreType.DMA
    out, momentum = pl.pallas_call(
        kernel,
        out_shape=(jax.ShapeDtypeStruct(shape, f32),) * 2,
        in_specs=[pl.BlockSpec(memory_space=pltpu.HBM)] * 3,
        out_specs=[pl.BlockSpec(memory_space=pltpu.VMEM)] * 2,
        scratch_shapes=[
            vmem(shape, f32), vmem(shape, f32), vmem(shape, f32),
            vmem((4, ROWS, 128), f32),
            vmem((HALVES, NY, 128, 128), f32), vmem((HALVES, NZC, 64, 128), f32),
            vmem((HALVES, NZC, NY, 8, 128), f32), vmem((HALVES, NY, NZC, 8, 128), f32),
            vmem((2 * HALVES, 128, 1024), f32),
            vmem((2 * HALVES, 128, 128), f32), vmem((2 * HALVES, NX, 128, 128), f32),
            vmem((HALVES, NZC, NY, 8, 128), f32), vmem((HALVES, NY, NZC, 8, 128), f32),
            vmem((HALVES, NZC, NY, 8, 128), f32), vmem((HALVES, NY, NZC, 8, 128), f32),
            vmem((4, 128, 8, 128), f32),
            dma((2 * HALVES + 1, 2)),
            dma((12 * HALVES,)), dma((12 * HALVES,)),
            dma((2 * HALVES,)), dma((2 * HALVES,)),
        ],
        compiler_params=pltpu.CompilerParams(
            collective_id=0, has_side_effects=True, vmem_limit_bytes=48 * 1024 * 1024),
        name="exchange",
    )(flat(slopes_in), flat(moments_in), flat(weights_in))
    out, momentum = pl.pallas_call(
        land,
        out_shape=(jax.ShapeDtypeStruct(shape, f32),) * 2,
        in_specs=[pl.BlockSpec(memory_space=pltpu.VMEM)] * 2,
        out_specs=[pl.BlockSpec(memory_space=pltpu.HBM)] * 2,
        scratch_shapes=[dma((2, PIECES))],
        compiler_params=pltpu.CompilerParams(vmem_limit_bytes=16 * 1024 * 1024),
        name="land",
    )(out, momentum)
    return whole(out), whole(momentum)


def solution(mesh):
    spec = P(None, "zero", "width")
    return jax.shard_map(body, mesh=mesh, in_specs=(spec,) * 3, out_specs=(spec,) * 2, check_vma=False)
```

```python
import jax
import jax.numpy as jnp
from jax import lax
from jax.experimental import pallas as pl
from jax.experimental.pallas import tpu as pltpu
from jax.sharding import PartitionSpec as P

MESH = pl.DeviceIdType.MESH

hold_rate = 0.8
learn_rate = 0.8
decay_rate = 0.1

NX, NY, NZ, NC = 4, 8, 8, 2
NZC = NZ * NC
HALVES = 2
ROWS = 1024


def dot(a, b, contract):
    return lax.dot_general(
        a, b, (contract, ((), ())), precision=lax.Precision.HIGHEST, preferred_element_type=jnp.float32
    )


def ring_step(k, n):
    d = lax.div(n - k, 2)
    return d + lax.rem(k, 2) * (n - 2 * d)


def kernel(
    slopes, moments, weights, out, momentum,
    sl, mo, we, direct, t1, t2, r1, r2, xs, gs, gr, v1, v2, w1, w2, final,
    in_sem, send_sem, recv_sem, x_send, x_recv,
):
    zero = lax.axis_index("zero")
    width = lax.axis_index("width")
    core = lax.rem(zero, NC)
    y = lax.rem(lax.div(zero, NC), NY)
    zh = lax.div(zero, NC * NY)
    x = lax.rem(width, NX)
    own = lax.div(width, NX) * NC + core
    zc = zh * 4 + own

    def device(px, py, pzh, quarter):
        return ((pzh * NY + py) * NC + lax.rem(quarter, NC), lax.div(quarter, NC) * NX + px)

    def y_partner(k, back):
        d = ring_step(k, NY)
        return lax.rem(y + NY - d, NY) if back else lax.rem(y + d, NY)

    def z_partner(g, k, back):
        if g == 0:
            idx, quarter = 0, k
        elif g == 1:
            idx, quarter = 1 + 2 * lax.rem(k, 2), lax.div(k, 2)
        else:
            idx, quarter = 2, lax.rem(own + 1 + k, 4)
        return idx, quarter, lax.rem(zh + (idx + 2 if back else 6 - idx), 4)

    Z_FAR, Z_NEAR = ((0, 4),), ((1, 8), (2, 3))
    Z_ALL = Z_FAR + Z_NEAR
    Y_FAR, Y_NEAR = ((0, 3),), ((3, NY - 1),)
    Y_ALL = ((0, NY - 1),)

    def loop(lo, hi, step):
        def body(k, carry):
            step(k)
            return carry
        lax.fori_loop(lo, hi, body, 0)

    barrier = pltpu.get_barrier_semaphore()

    def greet(target):
        pl.semaphore_signal(barrier, inc=1, device_id=target, device_id_type=MESH)

    for d in (2, 1, 3, 0):
        pzh = lax.rem(zh + d, 4)
        for q in range(4):
            if d > 0:
                greet(device(x, y, pzh, q))
            elif q > 0:
                greet(device(x, y, pzh, lax.rem(own + q, 4)))
    for d in (4, 3, 5, 2, 6, 1, 7):
        greet(device(x, lax.rem(y + d, NY), zh, own))
    for d in (2, 1, 3):
        greet(device(lax.rem(x + d, NX), y, zh, own))

    loads = []
    for u in range(2 * HALVES):
        rows = pl.ds(u * ROWS, ROWS)
        loads.append((
            pltpu.make_async_copy(slopes.at[rows], sl.at[rows], in_sem.at[u, 0]),
            pltpu.make_async_copy(moments.at[rows], mo.at[rows], in_sem.at[u, 1]),
        ))
    for a, b in loads:
        a.start()
        b.start()

    load_weights = pltpu.make_async_copy(weights, we, in_sem.at[2 * HALVES, 0])
    load_weights.start()

    def remote(s, src, dst, target):
        return pltpu.make_async_remote_copy(
            src_ref=src, dst_ref=dst, send_sem=send_sem.at[s], recv_sem=recv_sem.at[s],
            device_id=target, device_id_type=MESH)

    class Along:
        def __init__(self, axis, s, groups, back, src, dst, whole):
            self.axis, self.s, self.groups, self.back = axis, s, groups, back
            self.src, self.dst, self.whole = src, dst, whole

        def copy(self, g, k):
            if self.axis == "y":
                p = y_partner(k, self.back)
                return remote(self.s, self.src(k, p), self.dst(k), device(x, p, zh, own))
            idx, quarter, pzh = z_partner(g, k, self.back)
            return remote(self.s, self.src(idx * 4 + quarter, pzh * 4 + quarter), self.dst(idx * 4 + own),
                          device(x, y, pzh, quarter))

        def start(self):
            for g, n in self.groups:
                if self.axis == "y":
                    loop(g, n, lambda k: self.copy(0, k).start())
                else:
                    loop(0, n, lambda k: self.copy(g, k).start())

        def all(self):
            return remote(self.s, self.whole, self.whole, device(x, lax.rem(y + 1, NY), zh, own))

    def x_copy(s, px):
        return pltpu.make_async_remote_copy(
            src_ref=gs.at[s], dst_ref=gr.at[s, x], send_sem=x_send.at[s], recv_sem=x_recv.at[s],
            device_id=device(px, y, zh, own), device_id_type=MESH)

    def x_all(s):
        whole = gr.at[s, pl.ds(0, NX - 1)]
        return pltpu.make_async_remote_copy(
            src_ref=whole, dst_ref=whole, send_sem=x_send.at[s], recv_sem=x_recv.at[s],
            device_id=device(lax.rem(x + 1, NX), y, zh, own), device_id_type=MESH)

    out1, out2, back1, back2 = [], [], [], []
    for h in range(HALVES):
        a, b = 2 * h, 2 * h + 1
        out1.append((
            Along("y", 12 * h, Y_ALL, False, lambda k, p, a=a: direct.at[a, pl.ds(p * 128, 128)],
                  lambda k, h=h: t1.at[h, k], t1.at[h, pl.ds(0, NY - 1)]),
            Along("z", 12 * h + 1, Z_ALL, False, lambda k, p, b=b: direct.at[b, pl.ds(p * 64, 64)],
                  lambda k, h=h: t2.at[h, k], t2.at[h, pl.ds(0, NZC - 1)]),
        ))
        out2.append((
            Along("z", 12 * h + 2, Z_ALL, False, lambda k, p, h=h: t1.at[h, :, pl.ds(p * 8, 8)],
                  lambda k, h=h: r1.at[h, zc], r1.at[h, pl.ds(0, NZC - 1)]),
            Along("y", 12 * h + 3, Y_ALL, False, lambda k, p, h=h: t2.at[h, :, pl.ds(p * 8, 8)],
                  lambda k, h=h: r2.at[h, y], r2.at[h, pl.ds(0, NY - 1)]),
        ))
        back1.append([])
        back2.append([])
        for part in range(2):
            ya, yb = (pl.ds(0, 3), pl.ds(3, 5))[part], (pl.ds(0, 4), pl.ds(4, 12))[part]
            s = 12 * h + 4 + 4 * part
            back1[h].append((
                Along("z", s, Z_ALL, False, lambda k, p, h=h, ya=ya: v1.at[h, p, ya],
                      lambda k, h=h, ya=ya: w1.at[h, zc, ya], w1.at[h, pl.ds(0, NZC - 1), ya]),
                Along("y", s + 1, Y_ALL, False, lambda k, p, h=h, yb=yb: v2.at[h, p, yb],
                      lambda k, h=h, yb=yb: w2.at[h, y, yb], w2.at[h, pl.ds(0, NY - 1), yb]),
            ))
            back2[h].append((
                Along("y", s + 2, (Y_FAR, Y_NEAR)[part], True, lambda k, p, h=h: w1.at[h, :, k],
                      lambda k, a=a: final.at[a, pl.ds(y * 16, 16)], final.at[a, pl.ds(0, (48, 64)[part])]),
                Along("z", s + 3, (Z_FAR, Z_NEAR)[part], True, lambda k, p, h=h: w2.at[h, :, k],
                      lambda k, b=b: final.at[b, pl.ds(zc * 8, 8)], final.at[b, pl.ds(0, (32, 88)[part])]),
            ))

    def take(h, i):
        flat = (r1, r2)[i].at[h].reshape(ROWS, 128)
        for zl in range(2):
            for ct in range(4):
                columns = pl.ds((zl * 4 + ct) * 128, 128)
                for row in range(2):
                    for zh in range(4):
                        if i == 0:
                            xs[2 * h, pl.ds(row * 64 + zh * 16, 16), columns] = flat[
                                pl.ds(zh * 256 + zl * 128 + ct * 2 + row, 16, stride=8), :]
                        else:
                            for c in range(2):
                                xs[2 * h + 1, pl.ds(row * 64 + zh * 16 + c * 8, 8), columns] = flat[
                                    pl.ds(zh * 32 + zl * 16 + c * 8 + ct * 2 + row, 8, stride=128), :]

    def give(h, i, new):
        flat = (v1, v2)[i].at[h].reshape(ROWS, 128)
        for zl in range(2):
            for ct in range(4):
                tile = new[:, (zl * 4 + ct) * 128:(zl * 4 + ct + 1) * 128]
                for row in range(2):
                    for zh in range(4):
                        first = row * 64 + zh * 16
                        if i == 0:
                            flat[pl.ds(zh * 256 + zl * 128 + ct * 2 + row, 16, stride=8), :] = tile[first:first + 16]
                        else:
                            for c in range(2):
                                flat[pl.ds(zh * 32 + zl * 16 + c * 8 + ct * 2 + row, 8, stride=128), :] = tile[
                                    first + c * 8:first + c * 8 + 8]

    def renew(u, first, rows):
        at = pl.ds(pl.multiple_of(u * ROWS + first, 8), rows)
        fresh = final[u, pl.ds(first // 8, rows // 8)].reshape(rows, 128)
        out[at, :] = (1.0 - learn_rate * decay_rate) * we[at, :] - learn_rate * fresh

    for u in range(2 * HALVES):
        loads[u][0].wait()
        loads[u][1].wait()
        rows = pl.ds(u * ROWS, ROWS)
        slope = sl[rows, :]
        fresh = hold_rate * mo[rows, :] + slope
        momentum[rows, :] = fresh
        direct[u] = hold_rate * fresh + slope
        if u == 0:
            pl.semaphore_wait(barrier, (NY - 1) + (NZC - 1) + (NX - 1))
        out1[u // 2][u % 2].start()
    for h in range(HALVES):
        t1[h, NY - 1] = direct[2 * h, pl.ds(pl.multiple_of(y * 128, 128), 128)]
        t2[h, 8 + own] = direct[2 * h + 1, pl.ds(pl.multiple_of(zc * 64, 64), 64)]

    for h in range(HALVES):
        for i in range(2):
            out1[h][i].all().wait_recv()
            out2[h][i].start()
        r1[h, zc] = t1[h, :, pl.ds(pl.multiple_of(zc * 8, 8), 8)]
        r2[h, y] = t2[h, :, pl.ds(pl.multiple_of(y * 8, 8), 8)]

    row_id = lax.broadcasted_iota(jnp.int32, (128, 128), 0)
    col_id = lax.broadcasted_iota(jnp.int32, (128, 128), 1)
    eye = (row_id == col_id).astype(jnp.float32)
    inner = ((1,), (0,))

    low_lanes = col_id[:32] < 64

    def pack(gram):
        corner = jnp.where(low_lanes, pltpu.roll(gram[64:96], 64, 1), gram[96:])
        return jnp.concatenate([gram[:64], corner], axis=0)

    def unpack(packed):
        corner = packed[64:]
        corner = jnp.concatenate([pltpu.roll(corner, 64, 1), corner], axis=0)
        mirrored = jnp.concatenate([packed[:64], jnp.zeros((64, 128), jnp.float32)], axis=0).T
        lower = jnp.where(col_id[:64] < 64, mirrored[64:], corner)
        return jnp.concatenate([packed[:64], lower], axis=0)

    def forward(h):
        for part in range(2):
            for i in range(2):
                back1[h][part][i].all().wait_recv()
                back2[h][part][i].start()

    for h in range(HALVES):
        for i in range(2):
            out2[h][i].all().wait_recv()
            take(h, i)
            a = xs[2 * h + i]
            gs[2 * h + i] = pack(dot(a, a, ((1,), (1,))))
            for k in (2, 1, 3):
                x_copy(2 * h + i, lax.rem(x + k, NX)).start()
            gr[2 * h + i, x] = gs[2 * h + i]
        if h > 0:
            forward(h - 1)
        grams, scales, totals = [], [], []
        for i in range(2):
            at = 2 * h + i
            x_all(at).wait_recv()
            gram = unpack((gr[at, 0] + gr[at, 1]) + (gr[at, 2] + gr[at, 3]))
            scale = lax.rsqrt(jnp.sum(jnp.sum(gram * eye, axis=1, keepdims=True), axis=0, keepdims=True) + 1e-06)
            scales.append(scale)
            grams.append(gram * (scale * scale))
        for step in range(3):
            mixes = [3.4445 * eye - 4.775 * g + 2.0315 * dot(g, g, inner) for g in grams]
            if step == 0:
                totals = [s * m for s, m in zip(scales, mixes)]
            if step < 2:
                halves = [dot(m, g, inner) for m, g in zip(mixes, grams)]
                grams = [dot(a, m, inner) for a, m in zip(halves, mixes)]
            if step > 0:
                totals = [dot(m, t, inner) for m, t in zip(mixes, totals)]
        for i in range(2):
            give(h, i, dot(totals[i], xs[2 * h + i], inner))
            back1[h][0][i].start()
            if i == 0:
                w1[h, zc] = v1[h, zc]
            else:
                w2[h, y] = v2[h, y]
        for i in range(2):
            back1[h][1][i].start()

    forward(HALVES - 1)
    load_weights.wait()
    for g in range(HALVES):
        final[2 * g, pl.ds(y * 16, 16)] = w1[g, :, NY - 1]
        final[2 * g + 1, pl.ds(zc * 8, 8)] = w2[g, :, 8 + own]
        renew(2 * g, y * 128, 128)
    for g in range(HALVES):
        for pair in (out1[g], out2[g], back1[g][0], back1[g][1]):
            for one in pair:
                one.all().wait_send()
        for i in range(2):
            x_all(2 * g + i).wait_send()
    for g in range(HALVES):
        for part in range(2):
            back2[g][part][0].all().wait_recv()
            for lo, hi in (Y_FAR, Y_NEAR)[part]:
                loop(lo, hi, lambda k: renew(2 * g, y_partner(k, False) * 128, 128))
            back2[g][part][1].all().wait_recv()
            for idx in ((0,), (1, 3, 2))[part]:
                renew(2 * g + 1, lax.rem(zh + 6 - idx, 4) * 256, 256)
    for g in range(HALVES):
        for pair in back2[g]:
            for one in pair:
                one.all().wait_send()


PIECES = 4


def land(out, momentum, out_hbm, momentum_hbm, sem):
    copies = []
    for i in range(PIECES):
        rows = pl.ds(i * (out.shape[0] // PIECES), out.shape[0] // PIECES)
        copies.append(pltpu.make_async_copy(out.at[rows], out_hbm.at[rows], sem.at[0, i]))
        copies.append(pltpu.make_async_copy(momentum.at[rows], momentum_hbm.at[rows], sem.at[1, i]))
    for copy in copies:
        copy.start()
    for copy in copies:
        copy.wait()


def body(slopes_in, moments_in, weights_in):
    mats, side, wide = slopes_in.shape

    def flat(a):
        return a.reshape(mats, side, wide // 128, 128).transpose(0, 2, 1, 3).reshape(mats * side * wide // 128, 128)

    def whole(a):
        return a.reshape(mats, wide // 128, side, 128).transpose(0, 2, 1, 3).reshape(mats, side, wide)

    f32 = jnp.float32
    shape = (mats * side * wide // 128, 128)
    vmem = pltpu.VMEM
    dma = pltpu.SemaphoreType.DMA
    out, momentum = pl.pallas_call(
        kernel,
        out_shape=(jax.ShapeDtypeStruct(shape, f32),) * 2,
        in_specs=[pl.BlockSpec(memory_space=pltpu.HBM)] * 3,
        out_specs=[pl.BlockSpec(memory_space=pltpu.VMEM)] * 2,
        scratch_shapes=[
            vmem(shape, f32), vmem(shape, f32), vmem(shape, f32),
            vmem((4, ROWS, 128), f32),
            vmem((HALVES, NY, 128, 128), f32), vmem((HALVES, NZC, 64, 128), f32),
            vmem((HALVES, NZC, NY, 8, 128), f32), vmem((HALVES, NY, NZC, 8, 128), f32),
            vmem((2 * HALVES, 128, 1024), f32),
            vmem((2 * HALVES, 96, 128), f32), vmem((2 * HALVES, NX, 96, 128), f32),
            vmem((HALVES, NZC, NY, 8, 128), f32), vmem((HALVES, NY, NZC, 8, 128), f32),
            vmem((HALVES, NZC, NY, 8, 128), f32), vmem((HALVES, NY, NZC, 8, 128), f32),
            vmem((4, 128, 8, 128), f32),
            dma((2 * HALVES + 1, 2)),
            dma((12 * HALVES,)), dma((12 * HALVES,)),
            dma((2 * HALVES,)), dma((2 * HALVES,)),
        ],
        compiler_params=pltpu.CompilerParams(
            collective_id=0, has_side_effects=True, vmem_limit_bytes=48 * 1024 * 1024),
        name="exchange",
    )(flat(slopes_in), flat(moments_in), flat(weights_in))
    out, momentum = pl.pallas_call(
        land,
        out_shape=(jax.ShapeDtypeStruct(shape, f32),) * 2,
        in_specs=[pl.BlockSpec(memory_space=pltpu.VMEM)] * 2,
        out_specs=[pl.BlockSpec(memory_space=pltpu.HBM)] * 2,
        scratch_shapes=[dma((2, PIECES))],
        compiler_params=pltpu.CompilerParams(vmem_limit_bytes=16 * 1024 * 1024),
        name="land",
    )(out, momentum)
    return whole(out), whole(momentum)


def solution(mesh):
    spec = P(None, "zero", "width")
    return jax.shard_map(body, mesh=mesh, in_specs=(spec,) * 3, out_specs=(spec,) * 2, check_vma=False)
```

```python
import jax
import jax.numpy as jnp
from jax import lax
from jax.experimental import pallas as pl
from jax.experimental.pallas import tpu as pltpu
from jax.sharding import PartitionSpec as P

MESH = pl.DeviceIdType.MESH

hold_rate = 0.8
learn_rate = 0.8
decay_rate = 0.1

NX, NY, NZ, NC = 4, 8, 8, 2
NZC = NZ * NC
HALVES = 2
ROWS = 1024


def dot(a, b, contract):
    return lax.dot_general(
        a, b, (contract, ((), ())), precision=lax.Precision.HIGHEST, preferred_element_type=jnp.float32
    )


def ring_step(k, n):
    d = lax.div(n - k, 2)
    return d + lax.rem(k, 2) * (n - 2 * d)


def kernel(
    slopes, moments, weights, out, momentum,
    sl, mo, we, direct, t1, t2, r1, r2, xs, gs, gr, v1, v2, w1, w2, final,
    in_sem, send_sem, recv_sem, x_send, x_recv,
):
    zero = lax.axis_index("zero")
    width = lax.axis_index("width")
    core = lax.rem(zero, NC)
    y = lax.rem(lax.div(zero, NC), NY)
    zh = lax.div(zero, NC * NY)
    x = lax.rem(width, NX)
    own = lax.div(width, NX) * NC + core
    zc = zh * 4 + own

    def device(px, py, pzh, quarter):
        return ((pzh * NY + py) * NC + lax.rem(quarter, NC), lax.div(quarter, NC) * NX + px)

    def y_partner(k, back):
        d = ring_step(k, NY)
        return lax.rem(y + NY - d, NY) if back else lax.rem(y + d, NY)

    def z_partner(g, k, back):
        if g == 0:
            idx, quarter = 0, k
        elif g == 1:
            idx, quarter = 1 + 2 * lax.rem(k, 2), lax.div(k, 2)
        else:
            idx, quarter = 2, lax.rem(own + 1 + k, 4)
        return idx, quarter, lax.rem(zh + (idx + 2 if back else 6 - idx), 4)

    Z_FAR, Z_NEAR = ((0, 4),), ((1, 8), (2, 3))
    Z_ALL = Z_FAR + Z_NEAR
    Y_FAR, Y_NEAR = ((0, 3),), ((3, NY - 1),)
    Y_ALL = ((0, NY - 1),)

    def loop(lo, hi, step):
        def body(k, carry):
            step(k)
            return carry
        lax.fori_loop(lo, hi, body, 0)

    loads = []
    for u in range(2 * HALVES):
        rows = pl.ds(u * ROWS, ROWS)
        loads.append((
            pltpu.make_async_copy(slopes.at[rows], sl.at[rows], in_sem.at[u, 0]),
            pltpu.make_async_copy(moments.at[rows], mo.at[rows], in_sem.at[u, 1]),
        ))
    for a, b in loads:
        a.start()
        b.start()

    barrier = pltpu.get_barrier_semaphore()

    def greet(target):
        pl.semaphore_signal(barrier, inc=1, device_id=target, device_id_type=MESH)

    for d in (2, 1, 3, 0):
        pzh = lax.rem(zh + d, 4)
        for q in range(4):
            if d > 0:
                greet(device(x, y, pzh, q))
            elif q > 0:
                greet(device(x, y, pzh, lax.rem(own + q, 4)))
    for d in (4, 3, 5, 2, 6, 1, 7):
        greet(device(x, lax.rem(y + d, NY), zh, own))
    for d in (2, 1, 3):
        greet(device(lax.rem(x + d, NX), y, zh, own))

    load_weights = pltpu.make_async_copy(weights, we, in_sem.at[2 * HALVES, 0])
    load_weights.start()

    def remote(s, src, dst, target):
        return pltpu.make_async_remote_copy(
            src_ref=src, dst_ref=dst, send_sem=send_sem.at[s], recv_sem=recv_sem.at[s],
            device_id=target, device_id_type=MESH)

    class Along:
        def __init__(self, axis, s, groups, back, src, dst, whole, near_first=False):
            self.axis, self.s, self.groups, self.back = axis, s, groups, back
            self.src, self.dst, self.whole, self.near_first = src, dst, whole, near_first

        def copy(self, g, k):
            if self.axis == "y":
                p = y_partner(k, self.back)
                return remote(self.s, self.src(k, p), self.dst(k), device(x, p, zh, own))
            idx, quarter, pzh = z_partner(g, k, self.back)
            return remote(self.s, self.src(idx * 4 + quarter, pzh * 4 + quarter), self.dst(idx * 4 + own),
                          device(x, y, pzh, quarter))

        def start(self):
            for g, n in self.groups[::-1] if self.near_first else self.groups:
                lo = g if self.axis == "y" else 0
                loop(lo, n, lambda k: self.copy(g, lo + n - 1 - k if self.near_first else k).start())

        def all(self):
            return remote(self.s, self.whole, self.whole, device(x, lax.rem(y + 1, NY), zh, own))

    def x_copy(s, px):
        return pltpu.make_async_remote_copy(
            src_ref=gs.at[s], dst_ref=gr.at[s, x], send_sem=x_send.at[s], recv_sem=x_recv.at[s],
            device_id=device(px, y, zh, own), device_id_type=MESH)

    def x_all(s):
        whole = gr.at[s, pl.ds(0, NX - 1)]
        return pltpu.make_async_remote_copy(
            src_ref=whole, dst_ref=whole, send_sem=x_send.at[s], recv_sem=x_recv.at[s],
            device_id=device(lax.rem(x + 1, NX), y, zh, own), device_id_type=MESH)

    out1, out2, back1, back2 = [], [], [], []
    for h in range(HALVES):
        a, b = 2 * h, 2 * h + 1
        out1.append((
            Along("y", 12 * h, Y_ALL, False, lambda k, p, a=a: direct.at[a, pl.ds(p * 128, 128)],
                  lambda k, h=h: t1.at[h, k], t1.at[h, pl.ds(0, NY - 1)]),
            Along("z", 12 * h + 1, Z_ALL, False, lambda k, p, b=b: direct.at[b, pl.ds(p * 64, 64)],
                  lambda k, h=h: t2.at[h, k], t2.at[h, pl.ds(0, NZC - 1)]),
        ))
        out2.append((
            Along("z", 12 * h + 2, Z_ALL, False, lambda k, p, h=h: t1.at[h, :, pl.ds(p * 8, 8)],
                  lambda k, h=h: r1.at[h, zc], r1.at[h, pl.ds(0, NZC - 1)], near_first=True),
            Along("y", 12 * h + 3, Y_ALL, False, lambda k, p, h=h: t2.at[h, :, pl.ds(p * 8, 8)],
                  lambda k, h=h: r2.at[h, y], r2.at[h, pl.ds(0, NY - 1)], near_first=True),
        ))
        back1.append([])
        back2.append([])
        for part in range(2):
            ya, yb = (pl.ds(0, 3), pl.ds(3, 5))[part], (pl.ds(0, 4), pl.ds(4, 12))[part]
            s = 12 * h + 4 + 4 * part
            back1[h].append((
                Along("z", s, Z_ALL, False, lambda k, p, h=h, ya=ya: v1.at[h, p, ya],
                      lambda k, h=h, ya=ya: w1.at[h, zc, ya], w1.at[h, pl.ds(0, NZC - 1), ya]),
                Along("y", s + 1, Y_ALL, False, lambda k, p, h=h, yb=yb: v2.at[h, p, yb],
                      lambda k, h=h, yb=yb: w2.at[h, y, yb], w2.at[h, pl.ds(0, NY - 1), yb]),
            ))
            back2[h].append((
                Along("y", s + 2, (Y_FAR, Y_NEAR)[part], True, lambda k, p, h=h: w1.at[h, :, k],
                      lambda k, a=a: final.at[a, pl.ds(y * 16, 16)], final.at[a, pl.ds(0, (48, 64)[part])]),
                Along("z", s + 3, (Z_FAR, Z_NEAR)[part], True, lambda k, p, h=h: w2.at[h, :, k],
                      lambda k, b=b: final.at[b, pl.ds(zc * 8, 8)], final.at[b, pl.ds(0, (32, 88)[part])]),
            ))

    def take(h, i):
        flat = (r1, r2)[i].at[h].reshape(ROWS, 128)
        for zl in range(2):
            for ct in range(4):
                columns = pl.ds((zl * 4 + ct) * 128, 128)
                for row in range(2):
                    for zh in range(4):
                        if i == 0:
                            xs[2 * h, pl.ds(row * 64 + zh * 16, 16), columns] = flat[
                                pl.ds(zh * 256 + zl * 128 + ct * 2 + row, 16, stride=8), :]
                        else:
                            for c in range(2):
                                xs[2 * h + 1, pl.ds(row * 64 + zh * 16 + c * 8, 8), columns] = flat[
                                    pl.ds(zh * 32 + zl * 16 + c * 8 + ct * 2 + row, 8, stride=128), :]

    def give(h, i, new):
        flat = (v1, v2)[i].at[h].reshape(ROWS, 128)
        for zl in range(2):
            for ct in range(4):
                tile = new[:, (zl * 4 + ct) * 128:(zl * 4 + ct + 1) * 128]
                for row in range(2):
                    for zh in range(4):
                        first = row * 64 + zh * 16
                        if i == 0:
                            flat[pl.ds(zh * 256 + zl * 128 + ct * 2 + row, 16, stride=8), :] = tile[first:first + 16]
                        else:
                            for c in range(2):
                                flat[pl.ds(zh * 32 + zl * 16 + c * 8 + ct * 2 + row, 8, stride=128), :] = tile[
                                    first + c * 8:first + c * 8 + 8]

    def renew(u, first, rows):
        at = pl.ds(pl.multiple_of(u * ROWS + first, 8), rows)
        fresh = final[u, pl.ds(first // 8, rows // 8)].reshape(rows, 128)
        out[at, :] = (1.0 - learn_rate * decay_rate) * we[at, :] - learn_rate * fresh

    for u in range(2 * HALVES):
        loads[u][0].wait()
        loads[u][1].wait()
        rows = pl.ds(u * ROWS, ROWS)
        slope = sl[rows, :]
        fresh = hold_rate * mo[rows, :] + slope
        momentum[rows, :] = fresh
        direct[u] = hold_rate * fresh + slope
        if u == 0:
            pl.semaphore_wait(barrier, (NY - 1) + (NZC - 1) + (NX - 1))
        out1[u // 2][u % 2].start()
    for h in range(HALVES):
        t1[h, NY - 1] = direct[2 * h, pl.ds(pl.multiple_of(y * 128, 128), 128)]
        t2[h, 8 + own] = direct[2 * h + 1, pl.ds(pl.multiple_of(zc * 64, 64), 64)]

    for h in range(HALVES):
        for i in range(2):
            out1[h][i].all().wait_recv()
            out2[h][i].start()
        r1[h, zc] = t1[h, :, pl.ds(pl.multiple_of(zc * 8, 8), 8)]
        r2[h, y] = t2[h, :, pl.ds(pl.multiple_of(y * 8, 8), 8)]

    row_id = lax.broadcasted_iota(jnp.int32, (128, 128), 0)
    col_id = lax.broadcasted_iota(jnp.int32, (128, 128), 1)
    eye = (row_id == col_id).astype(jnp.float32)
    inner = ((1,), (0,))

    low_lanes = col_id[:32] < 64

    def pack(gram):
        corner = jnp.where(low_lanes, pltpu.roll(gram[64:96], 64, 1), gram[96:])
        return jnp.concatenate([gram[:64], corner], axis=0)

    def unpack(packed):
        corner = packed[64:]
        corner = jnp.concatenate([pltpu.roll(corner, 64, 1), corner], axis=0)
        mirrored = jnp.concatenate([packed[:64], jnp.zeros((64, 128), jnp.float32)], axis=0).T
        lower = jnp.where(col_id[:64] < 64, mirrored[64:], corner)
        return jnp.concatenate([packed[:64], lower], axis=0)

    def forward(h):
        for part, i in ((0, 1), (0, 0), (1, 0), (1, 1)):
            back1[h][part][i].all().wait_recv()
            back2[h][part][i].start()

    for h in range(HALVES):
        for i in range(2):
            out2[h][i].all().wait_recv()
            take(h, i)
            a = xs[2 * h + i]
            gs[2 * h + i] = pack(dot(a, a, ((1,), (1,))))
            for k in (2, 1, 3):
                x_copy(2 * h + i, lax.rem(x + k, NX)).start()
            gr[2 * h + i, x] = gs[2 * h + i]
        if h > 0:
            forward(h - 1)
        grams, scales, totals = [], [], []
        for i in range(2):
            at = 2 * h + i
            x_all(at).wait_recv()
            gram = unpack((gr[at, 0] + gr[at, 1]) + (gr[at, 2] + gr[at, 3]))
            scale = lax.rsqrt(jnp.sum(jnp.sum(gram * eye, axis=1, keepdims=True), axis=0, keepdims=True) + 1e-06)
            scales.append(scale)
            grams.append(gram * (scale * scale))
        for step in range(3):
            mixes = [3.4445 * eye - 4.775 * g + 2.0315 * dot(g, g, inner) for g in grams]
            if step == 0:
                totals = [s * m for s, m in zip(scales, mixes)]
            if step < 2:
                halves = [dot(m, g, inner) for m, g in zip(mixes, grams)]
                grams = [dot(a, m, inner) for a, m in zip(halves, mixes)]
            if step > 0:
                totals = [dot(m, t, inner) for m, t in zip(mixes, totals)]
        for i in range(2):
            give(h, i, dot(totals[i], xs[2 * h + i], inner))
            back1[h][0][i].start()
            if i == 0:
                w1[h, zc] = v1[h, zc]
            else:
                w2[h, y] = v2[h, y]
        for i in range(2):
            back1[h][1][i].start()

    forward(HALVES - 1)
    load_weights.wait()
    for g in range(HALVES):
        final[2 * g, pl.ds(y * 16, 16)] = w1[g, :, NY - 1]
        final[2 * g + 1, pl.ds(zc * 8, 8)] = w2[g, :, 8 + own]
        renew(2 * g, y * 128, 128)
    for g in range(HALVES):
        for pair in (out1[g], out2[g], back1[g][0], back1[g][1]):
            for one in pair:
                one.all().wait_send()
        for i in range(2):
            x_all(2 * g + i).wait_send()
    for g in range(HALVES):
        for part in range(2):
            back2[g][part][0].all().wait_recv()
            for lo, hi in (Y_FAR, Y_NEAR)[part]:
                loop(lo, hi, lambda k: renew(2 * g, y_partner(k, False) * 128, 128))
            back2[g][part][1].all().wait_recv()
            for idx in ((0,), (1, 3, 2))[part]:
                renew(2 * g + 1, lax.rem(zh + 6 - idx, 4) * 256, 256)
    for g in range(HALVES):
        for pair in back2[g]:
            for one in pair:
                one.all().wait_send()


PIECES = 4


def land(out, momentum, out_hbm, momentum_hbm, sem):
    copies = []
    for i in range(PIECES):
        rows = pl.ds(i * (out.shape[0] // PIECES), out.shape[0] // PIECES)
        copies.append(pltpu.make_async_copy(out.at[rows], out_hbm.at[rows], sem.at[0, i]))
        copies.append(pltpu.make_async_copy(momentum.at[rows], momentum_hbm.at[rows], sem.at[1, i]))
    for copy in copies:
        copy.start()
    for copy in copies:
        copy.wait()


def body(slopes_in, moments_in, weights_in):
    mats, side, wide = slopes_in.shape

    def flat(a):
        return a.reshape(mats, side, wide // 128, 128).transpose(0, 2, 1, 3).reshape(mats * side * wide // 128, 128)

    def whole(a):
        return a.reshape(mats, wide // 128, side, 128).transpose(0, 2, 1, 3).reshape(mats, side, wide)

    f32 = jnp.float32
    shape = (mats * side * wide // 128, 128)
    vmem = pltpu.VMEM
    dma = pltpu.SemaphoreType.DMA
    out, momentum = pl.pallas_call(
        kernel,
        out_shape=(jax.ShapeDtypeStruct(shape, f32),) * 2,
        in_specs=[pl.BlockSpec(memory_space=pltpu.HBM)] * 3,
        out_specs=[pl.BlockSpec(memory_space=pltpu.VMEM)] * 2,
        scratch_shapes=[
            vmem(shape, f32), vmem(shape, f32), vmem(shape, f32),
            vmem((4, ROWS, 128), f32),
            vmem((HALVES, NY, 128, 128), f32), vmem((HALVES, NZC, 64, 128), f32),
            vmem((HALVES, NZC, NY, 8, 128), f32), vmem((HALVES, NY, NZC, 8, 128), f32),
            vmem((2 * HALVES, 128, 1024), f32),
            vmem((2 * HALVES, 96, 128), f32), vmem((2 * HALVES, NX, 96, 128), f32),
            vmem((HALVES, NZC, NY, 8, 128), f32), vmem((HALVES, NY, NZC, 8, 128), f32),
            vmem((HALVES, NZC, NY, 8, 128), f32), vmem((HALVES, NY, NZC, 8, 128), f32),
            vmem((4, 128, 8, 128), f32),
            dma((2 * HALVES + 1, 2)),
            dma((12 * HALVES,)), dma((12 * HALVES,)),
            dma((2 * HALVES,)), dma((2 * HALVES,)),
        ],
        compiler_params=pltpu.CompilerParams(
            collective_id=0, has_side_effects=True, vmem_limit_bytes=48 * 1024 * 1024),
        name="exchange",
    )(flat(slopes_in), flat(moments_in), flat(weights_in))
    out, momentum = pl.pallas_call(
        land,
        out_shape=(jax.ShapeDtypeStruct(shape, f32),) * 2,
        in_specs=[pl.BlockSpec(memory_space=pltpu.VMEM)] * 2,
        out_specs=[pl.BlockSpec(memory_space=pltpu.HBM)] * 2,
        scratch_shapes=[dma((2, PIECES))],
        compiler_params=pltpu.CompilerParams(vmem_limit_bytes=16 * 1024 * 1024),
        name="land",
    )(out, momentum)
    return whole(out), whole(momentum)


def solution(mesh):
    spec = P(None, "zero", "width")
    return jax.shard_map(body, mesh=mesh, in_specs=(spec,) * 3, out_specs=(spec,) * 2, check_vma=False)
```

```python
import jax
import jax.numpy as jnp
from jax import lax
from jax.experimental import pallas as pl
from jax.experimental.pallas import tpu as pltpu
from jax.sharding import PartitionSpec as P

MESH = pl.DeviceIdType.MESH

hold_rate = 0.8
learn_rate = 0.8
decay_rate = 0.1

NX, NY, NZ, NC = 4, 8, 8, 2
NZC = NZ * NC
HALVES = 2
ROWS = 1024


def dot(a, b, contract):
    return lax.dot_general(
        a, b, (contract, ((), ())), precision=lax.Precision.HIGHEST, preferred_element_type=jnp.float32
    )


def ring_step(k, n):
    d = lax.div(n - k, 2)
    return d + lax.rem(k, 2) * (n - 2 * d)


def kernel(
    slopes, moments, weights, out, momentum,
    sl, mo, we, direct, t1, t2, r1, r2, xs, gs, gr, v1, v2, w1, w2, final,
    in_sem, send_sem, recv_sem, x_send, x_recv,
):
    zero = lax.axis_index("zero")
    width = lax.axis_index("width")
    core = lax.rem(zero, NC)
    y = lax.rem(lax.div(zero, NC), NY)
    zh = lax.div(zero, NC * NY)
    x = lax.rem(width, NX)
    own = lax.div(width, NX) * NC + core
    zc = zh * 4 + own

    def device(px, py, pzh, quarter):
        return ((pzh * NY + py) * NC + lax.rem(quarter, NC), lax.div(quarter, NC) * NX + px)

    def y_partner(k, back):
        d = ring_step(k, NY)
        return lax.rem(y + NY - d, NY) if back else lax.rem(y + d, NY)

    def z_partner(g, k, back):
        if g == 0:
            idx, quarter = 0, k
        elif g == 1:
            idx, quarter = 1 + 2 * lax.rem(k, 2), lax.div(k, 2)
        else:
            idx, quarter = 2, lax.rem(own + 1 + k, 4)
        return idx, quarter, lax.rem(zh + (idx + 2 if back else 6 - idx), 4)

    Z_FAR, Z_NEAR = ((0, 4),), ((1, 8), (2, 3))
    Z_ALL = Z_FAR + Z_NEAR
    Y_FAR, Y_NEAR = ((0, 3),), ((3, NY - 1),)
    Y_ALL = ((0, NY - 1),)

    def loop(lo, hi, step):
        def body(k, carry):
            step(k)
            return carry
        lax.fori_loop(lo, hi, body, 0)

    loads = []
    for u in range(2 * HALVES):
        rows = pl.ds(u * ROWS, ROWS)
        loads.append((
            pltpu.make_async_copy(slopes.at[rows], sl.at[rows], in_sem.at[u, 0]),
            pltpu.make_async_copy(moments.at[rows], mo.at[rows], in_sem.at[u, 1]),
        ))
    for copy in loads[0]:
        copy.start()

    barrier = pltpu.get_barrier_semaphore()

    def greet(target):
        pl.semaphore_signal(barrier, inc=1, device_id=target, device_id_type=MESH)

    for d in (2, 1, 3, 0):
        pzh = lax.rem(zh + d, 4)
        for q in range(4):
            if d > 0:
                greet(device(x, y, pzh, q))
            elif q > 0:
                greet(device(x, y, pzh, lax.rem(own + q, 4)))
    for d in (4, 3, 5, 2, 6, 1, 7):
        greet(device(x, lax.rem(y + d, NY), zh, own))
    for d in (2, 1, 3):
        greet(device(lax.rem(x + d, NX), y, zh, own))

    for pair in loads[1:]:
        for copy in pair:
            copy.start()
    load_weights = pltpu.make_async_copy(weights, we, in_sem.at[2 * HALVES, 0])

    def remote(s, src, dst, target):
        return pltpu.make_async_remote_copy(
            src_ref=src, dst_ref=dst, send_sem=send_sem.at[s], recv_sem=recv_sem.at[s],
            device_id=target, device_id_type=MESH)

    class Along:
        def __init__(self, axis, s, groups, back, src, dst, whole, near_first=False):
            self.axis, self.s, self.groups, self.back = axis, s, groups, back
            self.src, self.dst, self.whole, self.near_first = src, dst, whole, near_first

        def copy(self, g, k):
            if self.axis == "y":
                p = y_partner(k, self.back)
                return remote(self.s, self.src(k, p), self.dst(k), device(x, p, zh, own))
            idx, quarter, pzh = z_partner(g, k, self.back)
            return remote(self.s, self.src(idx * 4 + quarter, pzh * 4 + quarter), self.dst(idx * 4 + own),
                          device(x, y, pzh, quarter))

        def start(self):
            for g, n in self.groups[::-1] if self.near_first else self.groups:
                lo = g if self.axis == "y" else 0
                loop(lo, n, lambda k: self.copy(g, lo + n - 1 - k if self.near_first else k).start())

        def all(self):
            return remote(self.s, self.whole, self.whole, device(x, lax.rem(y + 1, NY), zh, own))

    def x_copy(s, px):
        return pltpu.make_async_remote_copy(
            src_ref=gs.at[s], dst_ref=gr.at[s, x], send_sem=x_send.at[s], recv_sem=x_recv.at[s],
            device_id=device(px, y, zh, own), device_id_type=MESH)

    def x_all(s):
        whole = gr.at[s, pl.ds(0, NX - 1)]
        return pltpu.make_async_remote_copy(
            src_ref=whole, dst_ref=whole, send_sem=x_send.at[s], recv_sem=x_recv.at[s],
            device_id=device(lax.rem(x + 1, NX), y, zh, own), device_id_type=MESH)

    out1, out2, back1, back2 = [], [], [], []
    for h in range(HALVES):
        a, b = 2 * h, 2 * h + 1
        out1.append((
            Along("y", 12 * h, Y_ALL, False, lambda k, p, a=a: direct.at[a, pl.ds(p * 128, 128)],
                  lambda k, h=h: t1.at[h, k], t1.at[h, pl.ds(0, NY - 1)]),
            Along("z", 12 * h + 1, Z_ALL, False, lambda k, p, b=b: direct.at[b, pl.ds(p * 64, 64)],
                  lambda k, h=h: t2.at[h, k], t2.at[h, pl.ds(0, NZC - 1)]),
        ))
        out2.append((
            Along("z", 12 * h + 2, Z_ALL, False, lambda k, p, h=h: t1.at[h, :, pl.ds(p * 8, 8)],
                  lambda k, h=h: r1.at[h, zc], r1.at[h, pl.ds(0, NZC - 1)], near_first=True),
            Along("y", 12 * h + 3, Y_ALL, False, lambda k, p, h=h: t2.at[h, :, pl.ds(p * 8, 8)],
                  lambda k, h=h: r2.at[h, y], r2.at[h, pl.ds(0, NY - 1)], near_first=True),
        ))
        back1.append([])
        back2.append([])
        for part in range(2):
            ya, yb = (pl.ds(0, 3), pl.ds(3, 5))[part], (pl.ds(0, 4), pl.ds(4, 12))[part]
            s = 12 * h + 4 + 4 * part
            back1[h].append((
                Along("z", s, Z_ALL, False, lambda k, p, h=h, ya=ya: v1.at[h, p, ya],
                      lambda k, h=h, ya=ya: w1.at[h, zc, ya], w1.at[h, pl.ds(0, NZC - 1), ya]),
                Along("y", s + 1, Y_ALL, False, lambda k, p, h=h, yb=yb: v2.at[h, p, yb],
                      lambda k, h=h, yb=yb: w2.at[h, y, yb], w2.at[h, pl.ds(0, NY - 1), yb]),
            ))
            back2[h].append((
                Along("y", s + 2, (Y_FAR, Y_NEAR)[part], True, lambda k, p, h=h: w1.at[h, :, k],
                      lambda k, a=a: final.at[a, pl.ds(y * 16, 16)], final.at[a, pl.ds(0, (48, 64)[part])]),
                Along("z", s + 3, (Z_FAR, Z_NEAR)[part], True, lambda k, p, h=h: w2.at[h, :, k],
                      lambda k, b=b: final.at[b, pl.ds(zc * 8, 8)], final.at[b, pl.ds(0, (32, 88)[part])]),
            ))

    def take(h, i):
        flat = (r1, r2)[i].at[h].reshape(ROWS, 128)
        for zl in range(2):
            for ct in range(4):
                columns = pl.ds((zl * 4 + ct) * 128, 128)
                for row in range(2):
                    for zh in range(4):
                        if i == 0:
                            xs[2 * h, pl.ds(row * 64 + zh * 16, 16), columns] = flat[
                                pl.ds(zh * 256 + zl * 128 + ct * 2 + row, 16, stride=8), :]
                        else:
                            for c in range(2):
                                xs[2 * h + 1, pl.ds(row * 64 + zh * 16 + c * 8, 8), columns] = flat[
                                    pl.ds(zh * 32 + zl * 16 + c * 8 + ct * 2 + row, 8, stride=128), :]

    def give(h, i, new):
        flat = (v1, v2)[i].at[h].reshape(ROWS, 128)
        for zl in range(2):
            for ct in range(4):
                tile = new[:, (zl * 4 + ct) * 128:(zl * 4 + ct + 1) * 128]
                for row in range(2):
                    for zh in range(4):
                        first = row * 64 + zh * 16
                        if i == 0:
                            flat[pl.ds(zh * 256 + zl * 128 + ct * 2 + row, 16, stride=8), :] = tile[first:first + 16]
                        else:
                            for c in range(2):
                                flat[pl.ds(zh * 32 + zl * 16 + c * 8 + ct * 2 + row, 8, stride=128), :] = tile[
                                    first + c * 8:first + c * 8 + 8]

    def renew(u, first, rows):
        at = pl.ds(pl.multiple_of(u * ROWS + first, 8), rows)
        fresh = final[u, pl.ds(first // 8, rows // 8)].reshape(rows, 128)
        out[at, :] = (1.0 - learn_rate * decay_rate) * we[at, :] - learn_rate * fresh

    for u in range(2 * HALVES):
        loads[u][0].wait()
        loads[u][1].wait()
        rows = pl.ds(u * ROWS, ROWS)
        slope = sl[rows, :]
        fresh = hold_rate * mo[rows, :] + slope
        momentum[rows, :] = fresh
        direct[u] = hold_rate * fresh + slope
        if u == 0:
            pl.semaphore_wait(barrier, (NY - 1) + (NZC - 1) + (NX - 1))
        out1[u // 2][u % 2].start()
    load_weights.start()
    for h in range(HALVES):
        t1[h, NY - 1] = direct[2 * h, pl.ds(pl.multiple_of(y * 128, 128), 128)]
        t2[h, 8 + own] = direct[2 * h + 1, pl.ds(pl.multiple_of(zc * 64, 64), 64)]

    for h in range(HALVES):
        for i in range(2):
            out1[h][i].all().wait_recv()
            out2[h][i].start()
        r1[h, zc] = t1[h, :, pl.ds(pl.multiple_of(zc * 8, 8), 8)]
        r2[h, y] = t2[h, :, pl.ds(pl.multiple_of(y * 8, 8), 8)]

    row_id = lax.broadcasted_iota(jnp.int32, (128, 128), 0)
    col_id = lax.broadcasted_iota(jnp.int32, (128, 128), 1)
    eye = (row_id == col_id).astype(jnp.float32)
    inner = ((1,), (0,))

    low_lanes = col_id[:32] < 64

    def pack(gram):
        corner = jnp.where(low_lanes, pltpu.roll(gram[64:96], 64, 1), gram[96:])
        return jnp.concatenate([gram[:64], corner], axis=0)

    def unpack(packed):
        corner = packed[64:]
        corner = jnp.concatenate([pltpu.roll(corner, 64, 1), corner], axis=0)
        mirrored = jnp.concatenate([packed[:64], jnp.zeros((64, 128), jnp.float32)], axis=0).T
        lower = jnp.where(col_id[:64] < 64, mirrored[64:], corner)
        return jnp.concatenate([packed[:64], lower], axis=0)

    def forward(h):
        for part, i in ((0, 1), (0, 0), (1, 0), (1, 1)):
            back1[h][part][i].all().wait_recv()
            back2[h][part][i].start()

    for h in range(HALVES):
        for i in range(2):
            out2[h][i].all().wait_recv()
            take(h, i)
            a = xs[2 * h + i]
            gs[2 * h + i] = pack(dot(a, a, ((1,), (1,))))
            for k in (2, 1, 3):
                x_copy(2 * h + i, lax.rem(x + k, NX)).start()
            gr[2 * h + i, x] = gs[2 * h + i]
        if h > 0:
            forward(h - 1)
        grams, scales, totals = [], [], []
        for i in range(2):
            at = 2 * h + i
            x_all(at).wait_recv()
            gram = unpack((gr[at, 0] + gr[at, 1]) + (gr[at, 2] + gr[at, 3]))
            scale = lax.rsqrt(jnp.sum(jnp.sum(gram * eye, axis=1, keepdims=True), axis=0, keepdims=True) + 1e-06)
            scales.append(scale)
            grams.append(gram * (scale * scale))
        for step in range(3):
            mixes = [3.4445 * eye - 4.775 * g + 2.0315 * dot(g, g, inner) for g in grams]
            if step == 0:
                totals = [s * m for s, m in zip(scales, mixes)]
            if step < 2:
                halves = [dot(m, g, inner) for m, g in zip(mixes, grams)]
                grams = [dot(a, m, inner) for a, m in zip(halves, mixes)]
            if step > 0:
                totals = [dot(m, t, inner) for m, t in zip(mixes, totals)]
        news = [dot(totals[i], xs[2 * h + i], inner) for i in range(2)]
        for i in range(2):
            give(h, i, news[i])
            back1[h][0][i].start()
            if i == 0:
                w1[h, zc] = v1[h, zc]
            else:
                w2[h, y] = v2[h, y]
        for i in range(2):
            back1[h][1][i].start()

    forward(HALVES - 1)
    load_weights.wait()
    for g in range(HALVES):
        final[2 * g, pl.ds(y * 16, 16)] = w1[g, :, NY - 1]
        final[2 * g + 1, pl.ds(zc * 8, 8)] = w2[g, :, 8 + own]
        renew(2 * g, y * 128, 128)
    for g in range(HALVES):
        for pair in (out1[g], out2[g], back1[g][0], back1[g][1]):
            for one in pair:
                one.all().wait_send()
        for i in range(2):
            x_all(2 * g + i).wait_send()
    for g in range(HALVES):
        for part in range(2):
            back2[g][part][0].all().wait_recv()
            for lo, hi in (Y_FAR, Y_NEAR)[part]:
                loop(lo, hi, lambda k: renew(2 * g, y_partner(k, False) * 128, 128))
            back2[g][part][1].all().wait_recv()
            for idx in ((0,), (1, 3, 2))[part]:
                renew(2 * g + 1, lax.rem(zh + 6 - idx, 4) * 256, 256)
    for g in range(HALVES):
        for pair in back2[g]:
            for one in pair:
                one.all().wait_send()


PIECES = 4


def land(out, momentum, out_hbm, momentum_hbm, sem):
    copies = []
    for i in range(PIECES):
        rows = pl.ds(i * (out.shape[0] // PIECES), out.shape[0] // PIECES)
        copies.append(pltpu.make_async_copy(out.at[rows], out_hbm.at[rows], sem.at[0, i]))
        copies.append(pltpu.make_async_copy(momentum.at[rows], momentum_hbm.at[rows], sem.at[1, i]))
    for copy in copies:
        copy.start()
    for copy in copies:
        copy.wait()


def body(slopes_in, moments_in, weights_in):
    mats, side, wide = slopes_in.shape

    def flat(a):
        return a.reshape(mats, side, wide // 128, 128).transpose(0, 2, 1, 3).reshape(mats * side * wide // 128, 128)

    def whole(a):
        return a.reshape(mats, wide // 128, side, 128).transpose(0, 2, 1, 3).reshape(mats, side, wide)

    f32 = jnp.float32
    shape = (mats * side * wide // 128, 128)
    vmem = pltpu.VMEM
    dma = pltpu.SemaphoreType.DMA
    out, momentum = pl.pallas_call(
        kernel,
        out_shape=(jax.ShapeDtypeStruct(shape, f32),) * 2,
        in_specs=[pl.BlockSpec(memory_space=pltpu.HBM)] * 3,
        out_specs=[pl.BlockSpec(memory_space=pltpu.VMEM)] * 2,
        scratch_shapes=[
            vmem(shape, f32), vmem(shape, f32), vmem(shape, f32),
            vmem((4, ROWS, 128), f32),
            vmem((HALVES, NY, 128, 128), f32), vmem((HALVES, NZC, 64, 128), f32),
            vmem((HALVES, NZC, NY, 8, 128), f32), vmem((HALVES, NY, NZC, 8, 128), f32),
            vmem((2 * HALVES, 128, 1024), f32),
            vmem((2 * HALVES, 96, 128), f32), vmem((2 * HALVES, NX, 96, 128), f32),
            vmem((HALVES, NZC, NY, 8, 128), f32), vmem((HALVES, NY, NZC, 8, 128), f32),
            vmem((HALVES, NZC, NY, 8, 128), f32), vmem((HALVES, NY, NZC, 8, 128), f32),
            vmem((4, 128, 8, 128), f32),
            dma((2 * HALVES + 1, 2)),
            dma((12 * HALVES,)), dma((12 * HALVES,)),
            dma((2 * HALVES,)), dma((2 * HALVES,)),
        ],
        compiler_params=pltpu.CompilerParams(
            collective_id=0, has_side_effects=True, vmem_limit_bytes=48 * 1024 * 1024),
        name="exchange",
    )(flat(slopes_in), flat(moments_in), flat(weights_in))
    out, momentum = pl.pallas_call(
        land,
        out_shape=(jax.ShapeDtypeStruct(shape, f32),) * 2,
        in_specs=[pl.BlockSpec(memory_space=pltpu.VMEM)] * 2,
        out_specs=[pl.BlockSpec(memory_space=pltpu.HBM)] * 2,
        scratch_shapes=[dma((2, PIECES))],
        compiler_params=pltpu.CompilerParams(vmem_limit_bytes=16 * 1024 * 1024),
        name="land",
    )(out, momentum)
    return whole(out), whole(momentum)


def solution(mesh):
    spec = P(None, "zero", "width")
    return jax.shard_map(body, mesh=mesh, in_specs=(spec,) * 3, out_specs=(spec,) * 2, check_vma=False)
```

```python
import jax
import jax.numpy as jnp
from jax import lax
from jax.experimental import pallas as pl
from jax.experimental.pallas import tpu as pltpu
from jax.sharding import PartitionSpec as P

MESH = pl.DeviceIdType.MESH

hold_rate = 0.8
learn_rate = 0.8
decay_rate = 0.1

NX, NY, NZ, NC = 4, 8, 8, 2
NZC = NZ * NC
HALVES = 2
ROWS = 1024


def dot(a, b, contract):
    return lax.dot_general(
        a, b, (contract, ((), ())), precision=lax.Precision.HIGHEST, preferred_element_type=jnp.float32
    )


def ring_step(k, n):
    d = lax.div(n - k, 2)
    return d + lax.rem(k, 2) * (n - 2 * d)


def kernel(
    slopes, moments, weights, out, momentum,
    sl, mo, we, direct, t1, t2, r1, r2, xs, gs, gr, v1, v2, w1, w2, final,
    in_sem, send_sem, recv_sem, x_send, x_recv,
):
    zero = lax.axis_index("zero")
    width = lax.axis_index("width")
    core = lax.rem(zero, NC)
    y = lax.rem(lax.div(zero, NC), NY)
    zh = lax.div(zero, NC * NY)
    x = lax.rem(width, NX)
    own = lax.div(width, NX) * NC + core
    zc = zh * 4 + own

    def device(px, py, pzh, quarter):
        return ((pzh * NY + py) * NC + lax.rem(quarter, NC), lax.div(quarter, NC) * NX + px)

    def y_partner(k, back):
        d = ring_step(k, NY)
        return lax.rem(y + NY - d, NY) if back else lax.rem(y + d, NY)

    def z_partner(g, k, back):
        if g == 0:
            idx, quarter = 0, k
        elif g == 1:
            idx, quarter = 1 + 2 * lax.rem(k, 2), lax.div(k, 2)
        else:
            idx, quarter = 2, lax.rem(own + 1 + k, 4)
        return idx, quarter, lax.rem(zh + (idx + 2 if back else 6 - idx), 4)

    Z_FAR, Z_NEAR = ((0, 4),), ((1, 8), (2, 3))
    Z_ALL = Z_FAR + Z_NEAR
    Y_FAR, Y_NEAR = ((0, 3),), ((3, NY - 1),)
    Y_ALL = ((0, NY - 1),)

    def loop(lo, hi, step):
        def body(k, carry):
            step(k)
            return carry
        lax.fori_loop(lo, hi, body, 0)

    loads = []
    for u in range(2 * HALVES):
        rows = pl.ds(u * ROWS, ROWS)
        loads.append((
            pltpu.make_async_copy(slopes.at[rows], sl.at[rows], in_sem.at[u, 0]),
            pltpu.make_async_copy(moments.at[rows], mo.at[rows], in_sem.at[u, 1]),
        ))
    for a, b in loads:
        a.start()
        b.start()

    barrier = pltpu.get_barrier_semaphore()

    def greet(target):
        pl.semaphore_signal(barrier, inc=1, device_id=target, device_id_type=MESH)

    for d in (2, 1, 3, 0):
        pzh = lax.rem(zh + d, 4)
        for q in range(4):
            if d > 0:
                greet(device(x, y, pzh, q))
            elif q > 0:
                greet(device(x, y, pzh, lax.rem(own + q, 4)))
    for d in (4, 3, 5, 2, 6, 1, 7):
        greet(device(x, lax.rem(y + d, NY), zh, own))
    for d in (2, 1, 3):
        greet(device(lax.rem(x + d, NX), y, zh, own))

    load_weights = pltpu.make_async_copy(weights, we, in_sem.at[2 * HALVES, 0])
    load_weights.start()

    def remote(s, src, dst, target):
        return pltpu.make_async_remote_copy(
            src_ref=src, dst_ref=dst, send_sem=send_sem.at[s], recv_sem=recv_sem.at[s],
            device_id=target, device_id_type=MESH)

    class Along:
        def __init__(self, axis, s, groups, back, src, dst, whole, near_first=False):
            self.axis, self.s, self.groups, self.back = axis, s, groups, back
            self.src, self.dst, self.whole, self.near_first = src, dst, whole, near_first

        def copy(self, g, k):
            if self.axis == "y":
                p = y_partner(k, self.back)
                return remote(self.s, self.src(k, p), self.dst(k), device(x, p, zh, own))
            idx, quarter, pzh = z_partner(g, k, self.back)
            return remote(self.s, self.src(idx * 4 + quarter, pzh * 4 + quarter), self.dst(idx * 4 + own),
                          device(x, y, pzh, quarter))

        def start(self):
            for g, n in self.groups[::-1] if self.near_first else self.groups:
                lo = g if self.axis == "y" else 0
                loop(lo, n, lambda k: self.copy(g, lo + n - 1 - k if self.near_first else k).start())

        def all(self):
            return remote(self.s, self.whole, self.whole, device(x, lax.rem(y + 1, NY), zh, own))

    def x_copy(s, px):
        return pltpu.make_async_remote_copy(
            src_ref=gs.at[s], dst_ref=gr.at[s, x], send_sem=x_send.at[s], recv_sem=x_recv.at[s],
            device_id=device(px, y, zh, own), device_id_type=MESH)

    def x_all(s):
        whole = gr.at[s, pl.ds(0, NX - 1)]
        return pltpu.make_async_remote_copy(
            src_ref=whole, dst_ref=whole, send_sem=x_send.at[s], recv_sem=x_recv.at[s],
            device_id=device(lax.rem(x + 1, NX), y, zh, own), device_id_type=MESH)

    out1, out2, back1, back2 = [], [], [], []
    for h in range(HALVES):
        a, b = 2 * h, 2 * h + 1
        out1.append((
            Along("y", 12 * h, Y_ALL, False, lambda k, p, a=a: direct.at[a, pl.ds(p * 128, 128)],
                  lambda k, h=h: t1.at[h, k], t1.at[h, pl.ds(0, NY - 1)]),
            Along("z", 12 * h + 1, Z_ALL, False, lambda k, p, b=b: direct.at[b, pl.ds(p * 64, 64)],
                  lambda k, h=h: t2.at[h, k], t2.at[h, pl.ds(0, NZC - 1)]),
        ))
        out2.append((
            Along("z", 12 * h + 2, Z_ALL, False, lambda k, p, h=h: t1.at[h, :, pl.ds(p * 8, 8)],
                  lambda k, h=h: r1.at[h, zc], r1.at[h, pl.ds(0, NZC - 1)], near_first=True),
            Along("y", 12 * h + 3, Y_ALL, False, lambda k, p, h=h: t2.at[h, :, pl.ds(p * 8, 8)],
                  lambda k, h=h: r2.at[h, y], r2.at[h, pl.ds(0, NY - 1)], near_first=True),
        ))
        back1.append([])
        back2.append([])
        for part in range(2):
            ya, yb = (pl.ds(0, 3), pl.ds(3, 5))[part], (pl.ds(0, 4), pl.ds(4, 12))[part]
            s = 12 * h + 4 + 4 * part
            back1[h].append((
                Along("z", s, Z_ALL, False, lambda k, p, h=h, ya=ya: v1.at[h, p, ya],
                      lambda k, h=h, ya=ya: w1.at[h, zc, ya], w1.at[h, pl.ds(0, NZC - 1), ya]),
                Along("y", s + 1, Y_ALL, False, lambda k, p, h=h, yb=yb: v2.at[h, p, yb],
                      lambda k, h=h, yb=yb: w2.at[h, y, yb], w2.at[h, pl.ds(0, NY - 1), yb]),
            ))
            back2[h].append((
                Along("y", s + 2, (Y_FAR, Y_NEAR)[part], True, lambda k, p, h=h: w1.at[h, :, k],
                      lambda k, a=a: final.at[a, pl.ds(y * 16, 16)], final.at[a, pl.ds(0, (48, 64)[part])]),
                Along("z", s + 3, (Z_FAR, Z_NEAR)[part], True, lambda k, p, h=h: w2.at[h, :, k],
                      lambda k, b=b: final.at[b, pl.ds(zc * 8, 8)], final.at[b, pl.ds(0, (32, 88)[part])]),
            ))

    def take(h, i):
        flat = (r1, r2)[i].at[h].reshape(ROWS, 128)
        for zl in range(2):
            for ct in range(4):
                columns = pl.ds((zl * 4 + ct) * 128, 128)
                for row in range(2):
                    for zh in range(4):
                        if i == 0:
                            xs[2 * h, pl.ds(row * 64 + zh * 16, 16), columns] = flat[
                                pl.ds(zh * 256 + zl * 128 + ct * 2 + row, 16, stride=8), :]
                        else:
                            for c in range(2):
                                xs[2 * h + 1, pl.ds(row * 64 + zh * 16 + c * 8, 8), columns] = flat[
                                    pl.ds(zh * 32 + zl * 16 + c * 8 + ct * 2 + row, 8, stride=128), :]

    def give(h, i, new):
        flat = (v1, v2)[i].at[h].reshape(ROWS, 128)
        for zl in range(2):
            for ct in range(4):
                tile = new[:, (zl * 4 + ct) * 128:(zl * 4 + ct + 1) * 128]
                for row in range(2):
                    for zh in range(4):
                        first = row * 64 + zh * 16
                        if i == 0:
                            flat[pl.ds(zh * 256 + zl * 128 + ct * 2 + row, 16, stride=8), :] = tile[first:first + 16]
                        else:
                            for c in range(2):
                                flat[pl.ds(zh * 32 + zl * 16 + c * 8 + ct * 2 + row, 8, stride=128), :] = tile[
                                    first + c * 8:first + c * 8 + 8]

    def renew(u, first, rows):
        at = pl.ds(pl.multiple_of(u * ROWS + first, 8), rows)
        fresh = final[u, pl.ds(first // 8, rows // 8)].reshape(rows, 128)
        out[at, :] = (1.0 - learn_rate * decay_rate) * we[at, :] - learn_rate * fresh

    for u in range(2 * HALVES):
        loads[u][0].wait()
        loads[u][1].wait()
        rows = pl.ds(u * ROWS, ROWS)
        slope = sl[rows, :]
        fresh = hold_rate * mo[rows, :] + slope
        momentum[rows, :] = fresh
        direct[u] = hold_rate * fresh + slope
        if u == 0:
            pl.semaphore_wait(barrier, (NY - 1) + (NZC - 1) + (NX - 1))
        out1[u // 2][u % 2].start()
    for h in range(HALVES):
        t1[h, NY - 1] = direct[2 * h, pl.ds(pl.multiple_of(y * 128, 128), 128)]
        t2[h, 8 + own] = direct[2 * h + 1, pl.ds(pl.multiple_of(zc * 64, 64), 64)]

    for h in range(HALVES):
        for i in range(2):
            out1[h][i].all().wait_recv()
            out2[h][i].start()
        r1[h, zc] = t1[h, :, pl.ds(pl.multiple_of(zc * 8, 8), 8)]
        r2[h, y] = t2[h, :, pl.ds(pl.multiple_of(y * 8, 8), 8)]

    row_id = lax.broadcasted_iota(jnp.int32, (128, 128), 0)
    col_id = lax.broadcasted_iota(jnp.int32, (128, 128), 1)
    eye = (row_id == col_id).astype(jnp.float32)
    inner = ((1,), (0,))

    low_lanes = col_id[:32] < 64

    def pack(gram):
        corner = jnp.where(low_lanes, pltpu.roll(gram[64:96], 64, 1), gram[96:])
        return jnp.concatenate([gram[:64], corner], axis=0)

    def unpack(packed):
        corner = packed[64:]
        corner = jnp.concatenate([pltpu.roll(corner, 64, 1), corner], axis=0)
        mirrored = jnp.concatenate([packed[:64], jnp.zeros((64, 128), jnp.float32)], axis=0).T
        lower = jnp.where(col_id[:64] < 64, mirrored[64:], corner)
        return jnp.concatenate([packed[:64], lower], axis=0)

    def forward(h):
        for part, i in ((0, 1), (0, 0), (1, 0), (1, 1)):
            back1[h][part][i].all().wait_recv()
            back2[h][part][i].start()

    for h in range(HALVES):
        for i in range(2):
            out2[h][i].all().wait_recv()
            take(h, i)
            a = xs[2 * h + i]
            gs[2 * h + i] = pack(dot(a, a, ((1,), (1,))))
            for k in (2, 1, 3):
                x_copy(2 * h + i, lax.rem(x + k, NX)).start()
            gr[2 * h + i, x] = gs[2 * h + i]
        if h > 0:
            forward(h - 1)
        grams, scales, totals = [], [], []
        for i in range(2):
            at = 2 * h + i
            x_all(at).wait_recv()
            gram = unpack((gr[at, 0] + gr[at, 1]) + (gr[at, 2] + gr[at, 3]))
            scale = lax.rsqrt(jnp.sum(jnp.sum(gram * eye, axis=1, keepdims=True), axis=0, keepdims=True) + 1e-06)
            scales.append(scale)
            grams.append(gram * (scale * scale))
        for step in range(3):
            mixes = [3.4445 * eye - 4.775 * g + 2.0315 * dot(g, g, inner) for g in grams]
            if step == 0:
                totals = [s * m for s, m in zip(scales, mixes)]
            if step < 2:
                halves = [dot(m, g, inner) for m, g in zip(mixes, grams)]
                grams = [dot(a, m, inner) for a, m in zip(halves, mixes)]
            if step == 1:
                totals = [dot(m, t, inner) for m, t in zip(mixes, totals)]
                partly = [dot(t, xs[2 * h + i], inner) for i, t in enumerate(totals)]
        for i in range(2):
            give(h, i, dot(mixes[i], partly[i], inner))
            back1[h][0][i].start()
            if i == 0:
                w1[h, zc] = v1[h, zc]
            else:
                w2[h, y] = v2[h, y]
        for i in range(2):
            back1[h][1][i].start()

    forward(HALVES - 1)
    load_weights.wait()
    for g in range(HALVES):
        final[2 * g, pl.ds(y * 16, 16)] = w1[g, :, NY - 1]
        final[2 * g + 1, pl.ds(zc * 8, 8)] = w2[g, :, 8 + own]
        renew(2 * g, y * 128, 128)
    for g in range(HALVES):
        for pair in (out1[g], out2[g], back1[g][0], back1[g][1]):
            for one in pair:
                one.all().wait_send()
        for i in range(2):
            x_all(2 * g + i).wait_send()
    for g in range(HALVES):
        for part in range(2):
            back2[g][part][0].all().wait_recv()
            for lo, hi in (Y_FAR, Y_NEAR)[part]:
                loop(lo, hi, lambda k: renew(2 * g, y_partner(k, False) * 128, 128))
            back2[g][part][1].all().wait_recv()
            for idx in ((0,), (1, 3, 2))[part]:
                renew(2 * g + 1, lax.rem(zh + 6 - idx, 4) * 256, 256)
    for g in range(HALVES):
        for pair in back2[g]:
            for one in pair:
                one.all().wait_send()


PIECES = 4


def land(out, momentum, out_hbm, momentum_hbm, sem):
    copies = []
    for i in range(PIECES):
        rows = pl.ds(i * (out.shape[0] // PIECES), out.shape[0] // PIECES)
        copies.append(pltpu.make_async_copy(out.at[rows], out_hbm.at[rows], sem.at[0, i]))
        copies.append(pltpu.make_async_copy(momentum.at[rows], momentum_hbm.at[rows], sem.at[1, i]))
    for copy in copies:
        copy.start()
    for copy in copies:
        copy.wait()


def body(slopes_in, moments_in, weights_in):
    mats, side, wide = slopes_in.shape

    def flat(a):
        return a.reshape(mats, side, wide // 128, 128).transpose(0, 2, 1, 3).reshape(mats * side * wide // 128, 128)

    def whole(a):
        return a.reshape(mats, wide // 128, side, 128).transpose(0, 2, 1, 3).reshape(mats, side, wide)

    f32 = jnp.float32
    shape = (mats * side * wide // 128, 128)
    vmem = pltpu.VMEM
    dma = pltpu.SemaphoreType.DMA
    out, momentum = pl.pallas_call(
        kernel,
        out_shape=(jax.ShapeDtypeStruct(shape, f32),) * 2,
        in_specs=[pl.BlockSpec(memory_space=pltpu.HBM)] * 3,
        out_specs=[pl.BlockSpec(memory_space=pltpu.VMEM)] * 2,
        scratch_shapes=[
            vmem(shape, f32), vmem(shape, f32), vmem(shape, f32),
            vmem((4, ROWS, 128), f32),
            vmem((HALVES, NY, 128, 128), f32), vmem((HALVES, NZC, 64, 128), f32),
            vmem((HALVES, NZC, NY, 8, 128), f32), vmem((HALVES, NY, NZC, 8, 128), f32),
            vmem((2 * HALVES, 128, 1024), f32),
            vmem((2 * HALVES, 96, 128), f32), vmem((2 * HALVES, NX, 96, 128), f32),
            vmem((HALVES, NZC, NY, 8, 128), f32), vmem((HALVES, NY, NZC, 8, 128), f32),
            vmem((HALVES, NZC, NY, 8, 128), f32), vmem((HALVES, NY, NZC, 8, 128), f32),
            vmem((4, 128, 8, 128), f32),
            dma((2 * HALVES + 1, 2)),
            dma((12 * HALVES,)), dma((12 * HALVES,)),
            dma((2 * HALVES,)), dma((2 * HALVES,)),
        ],
        compiler_params=pltpu.CompilerParams(
            collective_id=0, has_side_effects=True, vmem_limit_bytes=48 * 1024 * 1024),
        name="exchange",
    )(flat(slopes_in), flat(moments_in), flat(weights_in))
    out, momentum = pl.pallas_call(
        land,
        out_shape=(jax.ShapeDtypeStruct(shape, f32),) * 2,
        in_specs=[pl.BlockSpec(memory_space=pltpu.VMEM)] * 2,
        out_specs=[pl.BlockSpec(memory_space=pltpu.HBM)] * 2,
        scratch_shapes=[dma((2, PIECES))],
        compiler_params=pltpu.CompilerParams(vmem_limit_bytes=16 * 1024 * 1024),
        name="land",
    )(out, momentum)
    return whole(out), whole(momentum)


def solution(mesh):
    spec = P(None, "zero", "width")
    return jax.shard_map(body, mesh=mesh, in_specs=(spec,) * 3, out_specs=(spec,) * 2, check_vma=False)
```
